32 devices in a mesh: groups: 2 (over y), bank: 4 (over z), freq: 2 (over x), seg: 2 (over core).
Axes of the slice: x: 2, y: 2, z: 4, core: 2. Of those that a mesh axis runs over, the one named last changes fastest.
Arguments:
- coarse_spectra: bfloat16 [64, 2, 16384], P(('groups', 'seg', 'bank'), None, 'freq'), parts along dimension 0, may hold values from -6 to 6
- fine_spectra: bfloat16 [64, 2, 65536], P(('groups', 'seg', 'bank'), None, 'freq'), parts along dimension 0, may hold values from -6 to 6
- coarse_templates: bfloat16 [2, 2048, 16384], P(None, 'bank', 'freq'), may hold values from -6 to 6
- fine_templates: bfloat16 [2, 4, 64, 65536], P(None, 'bank', None, 'freq'), may hold values from -6 to 6
- coarse_weight: float32 [32768], P(('groups', 'freq')), parts along dimension 0, may hold values from 0.2 to 2
- fine_weight: float32 [131072], P(('groups', 'freq')), parts along dimension 0, may hold values from 0.2 to 2
- triggers: int32 [64, 2], P(('groups', 'seg')), parts along dimension 0, may hold values from 0 to 3, all different within a row; in each aligned block of 4 rows (0 to 3, 4 to 7, ...) at most 2 rows name the same one
- offsets: int32 [64, 2], P(('groups', 'seg')), parts along dimension 0, may hold values from 0 to 131056
Outputs:
- coarse_snr: float32 [2048, 64], P(('bank', 'freq'), ('groups', 'seg')), parts along dimension 1
- fine_snr: float32 [64, 2, 64], P(('groups', 'seg', 'bank'), None, 'freq'), parts along dimension 0
The draws below stay inside these ranges and needn't reach their ends.
There are 2 independent parts, one for each index of `groups`. The reference program is written for one: setup_inputs(seed, part) draws one part's arguments, and reference() takes and returns one part's arrays. A program takes and returns all parts, laid end to end along the dimension named above; an argument that names none is the same for every part. Nothing has to cross between parts.
Inputs may be any that keep to these rules, and one draw needn't show every extreme that they name: `triggers`: each segment names 2 different sub-banks. In each aligned block of 4 segments (the segments of one device along seg and bank) no sub-bank is named more than 2 times.
All inputs are finite; a program needn't handle non-finite values.
Results may differ from the reference program's by a relative error of at most 0.0021.
Values may be sent and summed in bfloat16 or wider, within the bound.
A program may use at most 128 MiB of HBM per device.

```python
import math
import jax
import jax.numpy as jnp
import numpy as np
from jax import lax

FC = 16384
FB = 65536
TC = 2048
TSUB = 64
SEG_DEV = 4
TOP = 2
CAP = 2
LC = 16
LF = 16
CSTRIDE = 2047
SUBBANKS = 4
SEGS = 32


def place_ends(values, rng, smallest, largest):
    spot = [jax.random.randint(jax.random.fold_in(rng, axis), (), 0, length) for axis, length in enumerate(values.shape)]
    main_axis = values.shape.index(max(values.shape))
    beside = spot[:main_axis] + [(spot[main_axis] + 1) % values.shape[main_axis]] + spot[main_axis + 1:]
    return values.at[tuple(spot)].set(smallest).at[tuple(beside)].set(largest)


def block_levels(stream_key, dims, shards, smallest, largest):
    loudness, own = 1.0, jax.random.fold_in(stream_key, 6)
    for position, parts in shards:
        steps = jnp.exp(jax.random.uniform(jax.random.fold_in(own, position), (parts,), jnp.float32, smallest / len(shards), largest / len(shards)))
        loudness = loudness * jnp.repeat(steps, dims[position] // parts).reshape([-1 if axis == position else 1 for axis in range(len(dims))])
    return loudness


def shared_out(stream_key, own, number, rows, count, top, reach, skew):
    ranking = jax.random.permutation(stream_key, count)
    packed, ordinary = portions_of(count, rows * top, reach, skew, True), portions_of(count, rows * top, reach, skew, False)
    places = jnp.arange(count)

    def named(lengths, rotation):
        used = int((lengths > 0).sum())
        fixed = max(1, used // 4)
        passed = fixed + (places - fixed + rotation * (used - fixed)) % max(1, count - fixed)
        return jnp.zeros((count,), jnp.int32).at[ranking[jnp.where(places < fixed, places, passed)]].set(jnp.asarray(lengths, jnp.int32))

    lengths = jnp.where(number % 4 == 0, named(packed, number // 4), named(ordinary, number - number // 4 - 1))
    mixed = jax.random.permutation(jax.random.fold_in(own, 3), count)
    source_of, sink = mixed[0:count // 2 * 2:2], mixed[1:count // 2 * 2:2]
    margin = jnp.minimum(lengths[source_of] - 1, reach - lengths[sink]) // 2
    margin = jnp.where((source_of == ranking[0]) | (sink == ranking[0]) | (lengths[sink] == 0), 0, jnp.maximum(margin, 0))
    passed = jax.random.randint(jax.random.fold_in(own, 4), (count // 2,), 0, 1 << 20) % (margin + 1)
    lengths = lengths.at[source_of].add(-passed).at[sink].add(passed)
    labels = jnp.searchsorted(jnp.cumsum(lengths), jnp.arange(rows * top), side="right").astype(jnp.int32)
    table = labels.reshape(top, rows).T
    table = table[jax.random.permutation(jax.random.fold_in(own, 1), rows)]
    rotation = jax.random.randint(jax.random.fold_in(own, 2), (rows, 1), 0, top)
    return jnp.take_along_axis(table, (jnp.arange(top)[None, :] + rotation) % top, axis=1)


def portions_of(amount, total, bound, skew, full):
    portions = [(1 << 20) // math.isqrt(standing ** skew) + 1 for standing in range(1, amount + 1)]
    largest = bound if full else min(bound, max(-(-total // amount), total * portions[0] // sum(portions)))
    least = 1 if total - largest >= amount - 1 else 0
    given, rest = [largest] + [least] * (amount - 1), total - largest - least * (amount - 1)
    while rest > 0:
        free = [i for i in range(1, amount) if given[i] < largest] or [i for i in range(1, amount) if given[i] < bound]
        pool, left = sum([portions[i] for i in free]), rest
        for i in free:
            addition = min(bound - given[i], max(1, left * portions[i] // pool), rest)
            given[i] = given[i] + addition
            rest = rest - addition
    return np.array(given)


def centred(rng, dims, width, limit, cuts=(), kind=jnp.bfloat16):
    array = width * jax.random.normal(rng, dims, jnp.float32)
    if cuts:
        array = array * block_levels(rng, dims, cuts, -0.22, 0.18)
    return jnp.clip(array, -limit, limit).astype(kind)


def setup_inputs(seed: int = 0, part: int = 0) -> dict:
    key_list = jax.random.split(jax.random.key(seed), 9)
    part_splits = jax.random.split(jax.random.fold_in(key_list[8], part), 9)
    coarse_spectra = centred(part_splits[0], (SEGS, 2, FC), 1.0, 6.0, ((0, 8), (2, 2)))
    fine_spectra = centred(part_splits[1], (SEGS, 2, FB), 1.0, 6.0, ((0, 8), (2, 2)))
    coarse_templates = centred(key_list[2], (2, TC, FC), 1.0, 6.0, ((1, 4), (2, 2)))
    fine_templates = centred(key_list[3], (2, SUBBANKS, TSUB, FB), 1.0, 6.0, ((1, 4), (3, 2)))
    coarse_weight = jnp.clip(jnp.exp(math.log(2.0) - 2.3025851 * jax.random.uniform(part_splits[4], (FC,), jnp.float32) ** block_levels(part_splits[4], (FC,), ((0, 2),), -0.2, 0.2)), 0.2, 2.0)
    fine_weight = jnp.clip(jnp.exp(math.log(2.0) - 2.3025851 * jax.random.uniform(part_splits[5], (FB,), jnp.float32) ** block_levels(part_splits[5], (FB,), ((0, 2),), -0.2, 0.2)), 0.2, 2.0)
    triggers_keys = jax.random.split(jax.random.fold_in(part_splits[6], 1), SEGS // SEG_DEV)
    triggers_turns = jax.random.permutation(jax.random.fold_in(part_splits[6], 3), SEGS // SEG_DEV)
    triggers = jax.vmap(lambda own, number: shared_out(jax.random.fold_in(part_splits[6], 2), own, number, SEG_DEV, SUBBANKS, TOP, CAP, 2))(triggers_keys, triggers_turns).reshape((SEGS, TOP))
    offsets = place_ends(jax.random.randint(part_splits[7], (SEGS, TOP), 0, 2 * FB - LF + 1), jax.random.fold_in(part_splits[7], 1), 0, 2 * FB - LF).astype(jnp.int32)
    return dict(coarse_spectra=coarse_spectra, fine_spectra=fine_spectra, coarse_templates=coarse_templates, fine_templates=fine_templates, coarse_weight=coarse_weight, fine_weight=fine_weight, triggers=triggers, offsets=offsets)


def phase_of(counts, period):
    radians = (2.0 * math.pi / period) * counts.astype(jnp.float32)
    return jnp.cos(radians), jnp.sin(radians)


def offset_count(freq_ids, offset, period):
    upper_bits = offset // 512
    lower_bits = offset % 512
    lower_term = (freq_ids * lower_bits) % period
    upper_term = ((freq_ids * upper_bits) % (period // 512)) * 512
    return (lower_term + upper_term) % period


def lagged(real_part, imag_part, lag_cos, lag_sin):
    left_real = real_part.T[:, :, None]
    left_imag = imag_part.T[:, :, None]
    right_cos = lag_cos[:, None, :]
    right_sin = lag_sin[:, None, :]
    lag_real = (left_real * right_cos - left_imag * right_sin).astype(jnp.bfloat16)
    lag_imag = (left_real * right_sin + left_imag * right_cos).astype(jnp.bfloat16)
    columns = real_part.shape[0] * lag_cos.shape[1]
    return lag_real.reshape(-1, columns), lag_imag.reshape(-1, columns)


def correlate(temp_real, temp_imag, lag_real, lag_imag):
    corr_real = jnp.dot(temp_real, lag_real, preferred_element_type=jnp.float32) + jnp.dot(temp_imag, lag_imag, preferred_element_type=jnp.float32)
    corr_imag = jnp.dot(temp_real, lag_imag, preferred_element_type=jnp.float32) - jnp.dot(temp_imag, lag_real, preferred_element_type=jnp.float32)
    return corr_real, corr_imag


def reference(coarse_spectra, fine_spectra, coarse_templates, fine_templates, coarse_weight, fine_weight, triggers, offsets):
    period_coarse = 2 * FC
    coarse_ids = jnp.arange(FC, dtype=jnp.int32)
    coarse_lags = jnp.arange(LC, dtype=jnp.int32) * CSTRIDE
    coarse_cos, coarse_sin = phase_of((coarse_ids[:, None] * coarse_lags[None, :]) % period_coarse, period_coarse)
    temp_real = coarse_templates[0]
    temp_imag = coarse_templates[1]
    coarse_norm = jnp.sum((temp_real.astype(jnp.float32) ** 2 + temp_imag.astype(jnp.float32) ** 2) * coarse_weight[None, :], axis=1)
    segment_blocks = coarse_spectra.reshape(SEGS // 8, 8, 2, FC)

    def coarse_block(segment_block):
        weighted = segment_block.astype(jnp.float32) * coarse_weight[None, None, :]
        lag_real, lag_imag = lagged(weighted[:, 0], weighted[:, 1], coarse_cos, coarse_sin)
        corr_real, corr_imag = correlate(temp_real, temp_imag, lag_real, lag_imag)
        energy = (corr_real * corr_real + corr_imag * corr_imag).reshape(TC, 8, LC)
        return jnp.max(energy, axis=2)

    peaks = lax.map(coarse_block, segment_blocks)
    coarse_snr = jnp.transpose(peaks, (1, 0, 2)).reshape(TC, SEGS) / coarse_norm[:, None]

    period_fine = 2 * FB
    fine_ids = jnp.arange(FB, dtype=jnp.int32)
    fine_lags = jnp.arange(LF, dtype=jnp.int32)
    fine_cos, fine_sin = phase_of((fine_ids[:, None] * fine_lags[None, :]) % period_fine, period_fine)
    fine_norm = jnp.sum((fine_templates[0].astype(jnp.float32) ** 2 + fine_templates[1].astype(jnp.float32) ** 2) * fine_weight[None, None, :], axis=2)
    pair_segments = jnp.repeat(jnp.arange(SEGS, dtype=jnp.int32), TOP)

    def fine_pair(pair):
        segment_id, bank_id, offset = pair
        spectrum = lax.dynamic_index_in_dim(fine_spectra, segment_id, 0, keepdims=False).astype(jnp.float32) * fine_weight[None, :]
        shift_cos, shift_sin = phase_of(offset_count(fine_ids, offset, period_fine), period_fine)
        shifted_real = spectrum[0] * shift_cos - spectrum[1] * shift_sin
        shifted_imag = spectrum[0] * shift_sin + spectrum[1] * shift_cos
        lag_real, lag_imag = lagged(shifted_real[None, :], shifted_imag[None, :], fine_cos, fine_sin)
        chosen = lax.dynamic_index_in_dim(fine_templates, bank_id, 1, keepdims=False)
        corr_real, corr_imag = correlate(chosen[0], chosen[1], lag_real, lag_imag)
        norm_row = lax.dynamic_index_in_dim(fine_norm, bank_id, 0, keepdims=False)
        return jnp.max(corr_real * corr_real + corr_imag * corr_imag, axis=1) / norm_row

    fine_rows = lax.map(fine_pair, (pair_segments, triggers.reshape(-1).astype(jnp.int32), offsets.reshape(-1).astype(jnp.int32)))
    return coarse_snr, fine_rows.reshape(SEGS, TOP, TSUB)
```

```python
import functools
import math

import jax
import jax.numpy as jnp
import numpy as np
from jax import lax
from jax.experimental import pallas as pl
from jax.experimental.pallas import tpu as pltpu
from jax.sharding import PartitionSpec as P

CAP = 2
LC = 16
LF = 16
CSTRIDE = 2047

MESH = pl.DeviceIdType.MESH
F32 = jnp.float32
BF16 = jnp.bfloat16
I32 = jnp.int32


def unit_table(count, stride, period):
    angle = 2.0 * np.pi * ((np.arange(count) * stride) % period) / period
    return np.stack([np.cos(angle), np.sin(angle)]).astype(np.float32)


def nt_dot(left, right):
    return lax.dot_general(left, right, (((1,), (1,)), ((), ())), preferred_element_type=F32)


def lag_series(real, imag, cos, sin, lags, emit):
    emit(0, real, imag)
    prev_re, prev_im = real, imag
    real, imag = real * cos - imag * sin, real * sin + imag * cos
    twice = cos + cos
    for j in range(1, lags):
        emit(j, real, imag)
        if j + 1 < lags:
            next_re = twice * real - prev_re
            next_im = twice * imag - prev_im
            prev_re, prev_im, real, imag = real, imag, next_re, next_im


def peak(energy, width):
    total = energy.shape[1]
    while total > width:
        half = total // 2
        if half % 128 == 0:
            energy = jnp.maximum(energy[:, :half], energy[:, half:])
        else:
            energy = jnp.maximum(energy, pltpu.roll(energy, energy.shape[1] - half, 1))
        total = half
    return energy


def kernel(cfg, *refs):
    nb, nf, kc, kf, chunks, period = cfg
    (
        trig, offs, coarse, fine, ctemp, ftemp, cweight, fweight, ctable, ftable,
        csnr, fout,
        coarse_v, fine_v, ctemp_v, ftemp_v, cw, fw, cstep, fstep,
        ag, outgoing, slots,
        cre0, cim0, cnre0, cre1, cim1, cnre1, fl0, fl1,
        cacc, cnorm, facc, fsum, fnorm, fsnr, back,
        crecv, cnrecv, frecv, fnrecv,
        in_sem, ct_sem, ft_sem,
        agr_send, agr_recv, agl_send, agl_recv, sl_send, sl_recv,
        cx_send, cx_recv, nx_send, nx_recv, fx_send, fx_recv, bk_send, bk_recv,
    ) = refs
    me = lax.axis_index("bank")
    fme = lax.axis_index("freq")
    seg_dev = coarse_v.shape[0]
    segs = nb * seg_dev
    rows = nb * CAP
    cbins = coarse_v.shape[2]
    fbins = fine_v.shape[2]
    csteps = cbins // kc
    fsteps = fbins // kf
    ctemps = ctemp_v.shape[1]
    sub_width = ftemp_v.shape[2]
    crow = ctemps // nf
    q = sub_width // nf
    nc = segs * LC
    nfl = rows * LF
    top_count = trig.shape[0]
    pairs = seg_dev * top_count
    cw_ag = cbins // chunks

    def win(i, width):
        return pl.ds(pl.multiple_of(i * width, width), width)

    small = [
        pltpu.make_async_copy(coarse, coarse_v, in_sem.at[0]),
        pltpu.make_async_copy(fine, fine_v, in_sem.at[1]),
        pltpu.make_async_copy(cweight, cw, in_sem.at[2]),
        pltpu.make_async_copy(fweight, fw, in_sem.at[3]),
        pltpu.make_async_copy(ctable.at[:, win(fme, cbins)], cstep, in_sem.at[4]),
        pltpu.make_async_copy(ftable.at[:, win(fme, fbins)], fstep, in_sem.at[5]),
    ]

    def ct_copy(i):
        return pltpu.make_async_copy(
            ctemp.at[:, :, win(i, kc)], ctemp_v.at[:, :, win(i, kc)], ct_sem.at[i]
        )

    def ft_copy(i):
        return pltpu.make_async_copy(
            ftemp.at[:, :, :, win(i, kf)], ftemp_v.at[:, :, :, win(i, kf)], ft_sem.at[i]
        )

    def ag_right(hop, chunk, block=None):
        block = me - hop if block is None else block
        view = ag.at[block, :, win(chunk, cw_ag)]
        return pltpu.make_async_remote_copy(
            src_ref=view, dst_ref=view,
            send_sem=agr_send.at[hop, chunk], recv_sem=agr_recv.at[hop, chunk],
            device_id={"bank": me + 1}, device_id_type=MESH,
        )

    def ag_left(hop, chunk, block=None):
        block = me + hop if block is None else block
        view = ag.at[block, :, win(chunk, cw_ag)]
        return pltpu.make_async_remote_copy(
            src_ref=view, dst_ref=view,
            send_sem=agl_send.at[hop, chunk], recv_sem=agl_recv.at[hop, chunk],
            device_id={"bank": me - 1}, device_id_type=MESH,
        )

    has_right = me + 1 < nb
    has_left = me >= 1

    def slot_copy(d, step):
        peer = lax.rem(me + d, nb)
        return pltpu.make_async_remote_copy(
            src_ref=outgoing.at[peer, :, win(step, kf)],
            dst_ref=slots.at[me, :, win(step, kf)],
            send_sem=sl_send.at[d - 1, step], recv_sem=sl_recv.at[d - 1, step],
            device_id={"bank": peer}, device_id_type=MESH,
        )

    def freq_copies(pairs_of, send, recv):
        copies = []
        for d in range(1, nf):
            peer = lax.rem(fme + d, nf)
            for k, (source, target) in enumerate(pairs_of):
                copies.append(
                    pltpu.make_async_remote_copy(
                        src_ref=source.at[peer], dst_ref=target.at[d - 1],
                        send_sem=send.at[d - 1, k], recv_sem=recv.at[d - 1, k],
                        device_id={"freq": peer}, device_id_type=MESH,
                    )
                )
        return copies

    def back_copies():
        return [
            pltpu.make_async_remote_copy(
                src_ref=fsnr, dst_ref=back.at[me],
                send_sem=bk_send.at[d - 1], recv_sem=bk_recv.at[d - 1],
                device_id={"bank": lax.rem(me + d, nb)}, device_id_type=MESH,
            )
            for d in range(1, nb)
        ]

    def by_part(block):
        block = block.astype(F32)
        return jnp.concatenate([block[:, 0, :], block[:, 1, :]], axis=0).astype(BF16)

    barrier = pltpu.get_barrier_semaphore()
    for d in range(1, nb):
        pl.semaphore_signal(
            barrier, inc=1, device_id={"bank": lax.rem(me + d, nb)}, device_id_type=MESH
        )
    for d in range(1, nf):
        pl.semaphore_signal(
            barrier, inc=1, device_id={"freq": lax.rem(fme + d, nf)}, device_id_type=MESH
        )
    for copy in small:
        copy.start()
    for i in range(csteps):
        ct_copy(i).start()
    for i in range(fsteps):
        ft_copy(i).start()
    small[0].wait()
    for c in range(chunks):
        ag[me, :, c * cw_ag : (c + 1) * cw_ag] = by_part(
            coarse_v[:, :, c * cw_ag : (c + 1) * cw_ag]
        )
    pl.semaphore_wait(barrier, nb - 1 + nf - 1)
    for c in range(chunks):

        @pl.when(has_right)
        def _():
            ag_right(0, c).start()

        @pl.when(has_left)
        def _():
            ag_left(0, c).start()

    own = [trig[p % top_count, me * seg_dev + p // top_count] for p in range(pairs)]

    def ranks_of(named):
        ranks = []
        for p in range(pairs):
            rank = jnp.int32(0)
            for before in range(p):
                rank = rank + (named[before] == named[p]).astype(I32)
            ranks.append(rank)
        return ranks

    own_rank = ranks_of(own)
    depth = 2 * CAP
    chooser_at = lax.broadcasted_iota(I32, (nb * depth, 2 * seg_dev), 0)
    chosen_col = jnp.zeros_like(chooser_at)
    for b in range(nb):
        for c in range(CAP):
            seg = jnp.int32(0)
            for p in range(pairs):
                hit = (own[p] == b) & (own_rank[p] == c)
                seg = jnp.where(hit, jnp.int32(p // top_count), seg)
            for part in range(2):
                chosen_col = jnp.where(
                    chooser_at == b * depth + part * CAP + c, seg + part * seg_dev, chosen_col
                )
    choice = jnp.where(
        lax.broadcasted_iota(I32, chooser_at.shape, 1) == chosen_col, 1.0, 0.0
    ).astype(BF16)

    small[1].wait()
    group = 2

    @pl.loop(0, fsteps // group)
    def _(i):
        for g in range(group):
            window = win(i * group + g, kf)
            chosen = jnp.dot(
                choice, by_part(fine_v[:, :, window]), preferred_element_type=F32
            ).astype(BF16)
            for b in range(nb):
                outgoing[b, :, window] = chosen[b * depth : (b + 1) * depth]

    slots[me] = outgoing[me]
    for copy in small[2:]:
        copy.wait()

    cnorm[...] = jnp.zeros_like(cnorm)
    fnorm[...] = jnp.zeros_like(fnorm)
    cacc[...] = jnp.zeros_like(cacc)
    facc[...] = jnp.zeros_like(facc)

    def coarse_norm(i):
        ct_copy(i).wait()
        weight = cw[:, win(i, kc)]
        step = 16
        for r in range(0, ctemps, step):
            part = None
            for c in range(0, kc, 128):
                lanes = pl.ds(pl.multiple_of(i * kc + c, 128), 128)
                hr = ctemp_v[0, r : r + step, lanes].astype(F32)
                hi = ctemp_v[1, r : r + step, lanes].astype(F32)
                term = (hr * hr + hi * hi) * weight[:, c : c + 128]
                part = term if part is None else part + term
            cnorm[r // crow, r % crow : r % crow + step, :] += part

    def fine_norm(i):
        ft_copy(i).wait()
        weight = fw[:, win(i, kf)]
        step = 16
        for r in range(0, sub_width, step):
            part = None
            for c in range(0, kf, 128):
                lanes = pl.ds(pl.multiple_of(i * kf + c, 128), 128)
                hr = ftemp_v[0, 0, r : r + step, lanes].astype(F32)
                hi = ftemp_v[1, 0, r : r + step, lanes].astype(F32)
                term = (hr * hr + hi * hi) * weight[:, c : c + 128]
                part = term if part is None else part + term
            fnorm[r // q, r % q : r % q + step, :] += part

    half = csteps // 2
    fillers = [(0, half, coarse_norm), (half, csteps, coarse_norm), (0, fsteps, fine_norm)]
    sent = 0
    for hop in range(nb - 1):
        if hop < len(fillers):
            low, high, fill = fillers[hop]
            pl.loop(low, high)(fill)
        for c in range(chunks):

            @pl.when(me - 1 - hop >= 0)
            def _():
                ag_right(hop, c, me - 1 - hop).wait_recv()

                @pl.when(has_right)
                def _():
                    ag_right(hop + 1, c).start()

            @pl.when(me + 1 + hop < nb)
            def _():
                ag_left(hop, c, me + 1 + hop).wait_recv()

                @pl.when(has_left)
                def _():
                    ag_left(hop + 1, c).start()

        upto = min(fsteps, sent + 2) if hop < nb - 2 else fsteps
        for step in range(sent, upto):
            for d in range(1, nb):
                slot_copy(d, step).start()
        sent = upto
    for low, high, fill in fillers[nb - 1 :]:
        pl.loop(low, high)(fill)
    norm_copies = freq_copies(((cnorm, cnrecv), (fnorm, fnrecv)), nx_send, nx_recv)
    for copy in norm_copies:
        copy.start()

    cbuf = ((cre0, cim0, cnre0), (cre1, cim1, cnre1))

    def coarse_lags(i, buf):
        re_ref, im_ref, nre_ref = buf
        sub = 256
        for c in range(0, kc, sub):
            window = pl.ds(pl.multiple_of(i * kc + c, sub), sub)
            blocks = [ag[b, :, window].astype(F32) for b in range(nb)]
            w = cw[:, window]
            real = jnp.concatenate([x[:seg_dev] for x in blocks], axis=0) * w
            imag = jnp.concatenate([x[seg_dev:] for x in blocks], axis=0) * w

            def emit(j, re, im):
                re = re.astype(BF16)
                re_ref[j * segs : (j + 1) * segs, c : c + sub] = re
                nre_ref[j * segs : (j + 1) * segs, c : c + sub] = -re
                im_ref[j * segs : (j + 1) * segs, c : c + sub] = im.astype(BF16)

            lag_series(real, imag, cstep[0:1, window], cstep[1:2, window], LC, emit)

    def coarse_products(i, buf):
        re_ref, im_ref, nre_ref = buf
        window = win(i, kc)
        left = jnp.concatenate([ctemp_v[0, :, window], ctemp_v[1, :, window]], axis=1)
        re, im, nre = re_ref[...], im_ref[...], nre_ref[...]
        right = jnp.concatenate(
            [jnp.concatenate([re, im], axis=1), jnp.concatenate([im, nre], axis=1)], axis=0
        )
        out = nt_dot(left, right)
        for k in range(nf):
            cacc[k] += out[k * crow : (k + 1) * crow]

    coarse_lags(0, cbuf[0])

    @pl.loop(0, csteps // 2)
    def _(i):
        coarse_lags(2 * i + 1, cbuf[1])
        coarse_products(2 * i, cbuf[0])
        coarse_lags(jnp.minimum(2 * i + 2, csteps - 1), cbuf[0])
        coarse_products(2 * i + 1, cbuf[1])

    coarse_copies = freq_copies(((cacc, crecv),), cx_send, cx_recv)
    for copy in coarse_copies:
        copy.start()

    row_at = lax.broadcasted_iota(I32, (rows, 128), 0)
    shift = jnp.zeros((rows, 128), I32)
    for b in range(nb):
        block = [trig[p % top_count, b * seg_dev + p // top_count] for p in range(pairs)]
        taken = jnp.int32(0)
        for p in range(pairs):
            hit = block[p] == me
            offset = offs[p % top_count, b * seg_dev + p // top_count]
            shift = jnp.where(
                row_at == jnp.where(hit, b * CAP + taken, -1), offset, shift
            )
            taken = taken + hit.astype(I32)
    lane = lax.broadcasted_iota(I32, (rows, 128), 1)
    tiles = fbins // 128
    lane_angle = ((shift * lane) & (period - 1)).astype(F32) * (2.0 * math.pi / period)
    lane_cos, lane_sin = jnp.cos(lane_angle), jnp.sin(lane_angle)
    coarse_period = period // 128
    tile_at = lax.broadcasted_iota(I32, (rows, tiles), 1) + fme * tiles
    wide = jnp.concatenate([shift] * (tiles // 128), axis=1)
    tile_angle = ((wide * tile_at) & (coarse_period - 1)).astype(F32) * (
        2.0 * math.pi / coarse_period
    )
    tile_cos, tile_sin = jnp.cos(tile_angle), jnp.sin(tile_angle)

    def fine_lags(i, buf):
        per = kf // 128
        turn = lax.rem(tiles - i * per, tiles)
        here_cos = pltpu.roll(tile_cos, turn, 1)
        here_sin = pltpu.roll(tile_sin, turn, 1)
        sub = 512
        for c in range(0, kf, sub):
            window = pl.ds(pl.multiple_of(i * kf + c, sub), sub)
            blocks = [slots[b, :, window].astype(F32) for b in range(nb)]
            w = fw[:, window]
            real = jnp.concatenate([x[:CAP] for x in blocks], axis=0) * w
            imag = jnp.concatenate([x[CAP:] for x in blocks], axis=0) * w
            turn_re, turn_im = [], []
            for t in range(c // 128, (c + sub) // 128):
                a_cos = here_cos[:, t : t + 1]
                a_sin = here_sin[:, t : t + 1]
                turn_re.append(a_cos * lane_cos - a_sin * lane_sin)
                turn_im.append(a_cos * lane_sin + a_sin * lane_cos)
            sr = jnp.concatenate(turn_re, axis=1)
            si = jnp.concatenate(turn_im, axis=1)
            real, imag = real * sr - imag * si, real * si + imag * sr
            held = []

            def emit(j, re, im):
                held.append((re, im))
                if len(held) == 2:
                    low, high = (j - 1) * rows, (j + 1) * rows
                    buf[low:high, c : c + sub] = jnp.concatenate(
                        [held[0][0], held[1][0]], axis=0
                    ).astype(BF16)
                    buf[nfl + low : nfl + high, c : c + sub] = jnp.concatenate(
                        [held[0][1], held[1][1]], axis=0
                    ).astype(BF16)
                    held.clear()

            lag_series(real, imag, fstep[0:1, window], fstep[1:2, window], LF, emit)

    def fine_products(i, buf):
        window = win(i, kf)
        left = jnp.concatenate([ftemp_v[0, 0, :, window], ftemp_v[1, 0, :, window]], axis=0)
        facc[...] += nt_dot(left, buf[...])

    def slots_here(step):
        for d in range(1, nb):
            slot_copy(d, step).wait_recv()

    slots_here(0)
    fine_lags(0, fl0)

    @pl.loop(0, fsteps // 2 - 1)
    def _(i):
        slots_here(2 * i + 1)
        slots_here(2 * i + 2)
        fine_lags(2 * i + 1, fl1)
        fine_products(2 * i, fl0)
        fine_lags(2 * i + 2, fl0)
        fine_products(2 * i + 1, fl1)

    slots_here(fsteps - 1)
    fine_lags(fsteps - 1, fl1)
    fine_products(fsteps - 2, fl0)
    fine_products(fsteps - 1, fl1)

    both = facc.shape[0] // 2
    re = facc[:both, :nfl] + facc[both:, nfl:]
    im = facc[:both, nfl:] - facc[both:, :nfl]
    for k in range(nf):
        fsum[k, 0] = re[k * q : (k + 1) * q]
        fsum[k, 1] = im[k * q : (k + 1) * q]
    fine_copies = freq_copies(((fsum, frecv),), fx_send, fx_recv)
    for copy in fine_copies:
        copy.start()
    for copy in norm_copies + fine_copies:
        copy.wait_recv()
    re, im, norm = fsum[fme, 0], fsum[fme, 1], fnorm[fme]
    for d in range(nf - 1):
        re = re + frecv[d, 0]
        im = im + frecv[d, 1]
        norm = norm + fnrecv[d]
    top = peak(re * re + im * im, rows)[:, :128]
    fsnr[...] = top / jnp.sum(norm, axis=1, keepdims=True)
    bcopies = back_copies()
    for copy in bcopies:
        copy.start()
    back[me] = fsnr[...]

    for copy in coarse_copies:
        copy.wait_recv()
    acc, norm = cacc[fme], cnorm[fme]
    for d in range(nf - 1):
        acc = acc + crecv[d]
        norm = norm + cnrecv[d]
    re, im = acc[:, :nc], acc[:, nc:]
    top = peak(re * re + im * im, segs)
    csnr[...] = jnp.transpose(top[:, :128] / jnp.sum(norm, axis=1, keepdims=True))[:segs]

    for copy in coarse_copies + norm_copies + fine_copies:
        copy.wait_send()
    for hop in range(nb - 1):
        for c in range(chunks):

            @pl.when(has_right & (me - hop >= 0))
            def _():
                ag_right(hop, c).wait_send()

            @pl.when(has_left & (me + hop < nb))
            def _():
                ag_left(hop, c).wait_send()

    @pl.loop(0, fsteps)
    def _(step):
        for d in range(1, nb):
            slot_copy(d, step).wait_send()

    for copy in bcopies:
        copy.wait()
    at = lax.broadcasted_iota(I32, back.shape[1:], 1)
    gathered = jnp.zeros(back.shape[1:], F32)
    for b in range(nb):
        turned = pltpu.roll(back[b], lax.rem((b - me + nb) * CAP + 128 - nb * CAP, 128), 1)
        gathered = jnp.where((at >= b * CAP) & (at < (b + 1) * CAP), turned, gathered)
    pair_at = lax.broadcasted_iota(I32, (pairs, 128), 0)
    place = jnp.zeros((pairs, 128), I32)
    for p in range(pairs):
        place = jnp.where(pair_at == p, own[p] * CAP + own_rank[p], place)
    giver = jnp.where(lax.broadcasted_iota(I32, (pairs, 128), 1) == place, 1.0, 0.0)
    fout[...] = lax.dot_general(
        giver, gathered, (((1,), (1,)), ((), ())),
        precision=lax.Precision.HIGHEST, preferred_element_type=F32,
    )


def body(
    coarse_spectra,
    fine_spectra,
    coarse_templates,
    fine_templates,
    coarse_weight,
    fine_weight,
    triggers,
    offsets,
):
    nb = lax.axis_size("bank")
    nf = lax.axis_size("freq")
    seg_local = fine_spectra.shape[0]
    cbins = coarse_spectra.shape[2]
    fbins = fine_spectra.shape[2]
    top_count = triggers.shape[1]
    sub_width = fine_templates.shape[2]
    ctemps = coarse_templates.shape[1]
    rows = nb * CAP
    segs = nb * seg_local
    kc = min(1024, cbins // 2)
    kf = min(2048, fbins // 2)
    chunks = 4
    csteps = cbins // kc
    fsteps = fbins // kf
    crow = ctemps // nf
    q = sub_width // nf
    period = 2 * fbins * nf
    assert period & (period - 1) == 0 and csteps % 2 == 0 and fsteps % 2 == 0
    nc = segs * LC
    nfl = rows * LF
    ctable = jnp.asarray(unit_table(cbins * nf, CSTRIDE, 2 * cbins * nf))
    ftable = jnp.asarray(unit_table(fbins * nf, 1, period))

    vmem, anywhere, scalar = (
        pl.BlockSpec(memory_space=pltpu.VMEM),
        pl.BlockSpec(memory_space=pl.ANY),
        pl.BlockSpec(memory_space=pltpu.SMEM),
    )
    dma = pltpu.SemaphoreType.DMA
    lag_buf = pltpu.VMEM((nc, kc), BF16)
    fine_buf = pltpu.VMEM((2 * nfl, kf), BF16)
    csnr, fine_rows = pl.pallas_call(
        functools.partial(kernel, (nb, nf, kc, kf, chunks, period)),
        out_shape=(
            jax.ShapeDtypeStruct((segs, crow), F32),
            jax.ShapeDtypeStruct((seg_local * top_count, q), F32),
        ),
        in_specs=[scalar, scalar] + [anywhere] * 8,
        out_specs=(vmem, vmem),
        scratch_shapes=[
            pltpu.VMEM(coarse_spectra.shape, BF16),
            pltpu.VMEM(fine_spectra.shape, BF16),
            pltpu.VMEM(coarse_templates.shape, BF16),
            pltpu.VMEM(fine_templates.shape, BF16),
            pltpu.VMEM((1, cbins), F32),
            pltpu.VMEM((1, fbins), F32),
            pltpu.VMEM((2, cbins), F32),
            pltpu.VMEM((2, fbins), F32),
            pltpu.VMEM((nb, 2 * seg_local, cbins), BF16),
            pltpu.VMEM((nb, 2 * CAP, fbins), BF16),
            pltpu.VMEM((nb, 2 * CAP, fbins), BF16),
            lag_buf, lag_buf, lag_buf, lag_buf, lag_buf, lag_buf,
            fine_buf, fine_buf,
            pltpu.VMEM((nf, crow, 2 * nc), F32),
            pltpu.VMEM((nf, crow, 128), F32),
            pltpu.VMEM((2 * sub_width, 2 * nfl), F32),
            pltpu.VMEM((nf, 2, q, nfl), F32),
            pltpu.VMEM((nf, q, 128), F32),
            pltpu.VMEM((q, 128), F32),
            pltpu.VMEM((nb, q, 128), F32),
            pltpu.VMEM((nf - 1, crow, 2 * nc), F32),
            pltpu.VMEM((nf - 1, crow, 128), F32),
            pltpu.VMEM((nf - 1, 2, q, nfl), F32),
            pltpu.VMEM((nf - 1, q, 128), F32),
            dma((6,)),
            dma((csteps,)),
            dma((fsteps,)),
            dma((nb - 1, chunks)),
            dma((nb - 1, chunks)),
            dma((nb - 1, chunks)),
            dma((nb - 1, chunks)),
            dma((nb - 1, fsteps)),
            dma((nb - 1, fsteps)),
            dma((nf - 1, 1)),
            dma((nf - 1, 1)),
            dma((nf - 1, 2)),
            dma((nf - 1, 2)),
            dma((nf - 1, 1)),
            dma((nf - 1, 1)),
            dma((nb - 1,)),
            dma((nb - 1,)),
        ],
        compiler_params=pltpu.CompilerParams(
            collective_id=0,
            has_side_effects=True,
            vmem_limit_bytes=60 * 1024 * 1024,
        ),
    )(
        triggers.T,
        offsets.T,
        coarse_spectra,
        fine_spectra,
        coarse_templates,
        fine_templates,
        coarse_weight[None, :],
        fine_weight[None, :],
        ctable,
        ftable,
    )
    return (csnr.T, fine_rows.reshape(seg_local, top_count, q))


def solution(mesh):
    return jax.shard_map(
        body,
        mesh=mesh,
        in_specs=(
            P(("groups", "seg", "bank"), None, "freq"),
            P(("groups", "seg", "bank"), None, "freq"),
            P(None, "bank", "freq"),
            P(None, "bank", None, "freq"),
            P(("groups", "freq")),
            P(("groups", "freq")),
            P(("groups", "seg"), None),
            P(("groups", "seg"), None),
        ),
        out_specs=(
            P(("bank", "freq"), ("groups", "seg")),
            P(("groups", "seg", "bank"), None, "freq"),
        ),
        check_vma=False,
    )
```

```python
import functools
import math

import jax
import jax.numpy as jnp
import numpy as np
from jax import lax
from jax.experimental import pallas as pl
from jax.experimental.pallas import tpu as pltpu
from jax.sharding import PartitionSpec as P

CAP = 2
LC = 16
LF = 16
CSTRIDE = 2047

MESH = pl.DeviceIdType.MESH
F32 = jnp.float32
BF16 = jnp.bfloat16
I32 = jnp.int32


def unit_table(count, stride, period):
    angle = 2.0 * np.pi * ((np.arange(count) * stride) % period) / period
    return np.stack([np.cos(angle), np.sin(angle)]).astype(np.float32)


def nt_dot(left, right):
    return lax.dot_general(left, right, (((1,), (1,)), ((), ())), preferred_element_type=F32)


def lag_series(real, imag, cos, sin, lags, emit):
    emit(0, real, imag)
    prev_re, prev_im = real, imag
    real, imag = real * cos - imag * sin, real * sin + imag * cos
    twice = cos + cos
    for j in range(1, lags):
        emit(j, real, imag)
        if j + 1 < lags:
            next_re = twice * real - prev_re
            next_im = twice * imag - prev_im
            prev_re, prev_im, real, imag = real, imag, next_re, next_im


def peak(energy, width):
    total = energy.shape[1]
    while total > width:
        half = total // 2
        if half % 128 == 0:
            energy = jnp.maximum(energy[:, :half], energy[:, half:])
        else:
            energy = jnp.maximum(energy, pltpu.roll(energy, energy.shape[1] - half, 1))
        total = half
    return energy


def kernel(cfg, *refs):
    nb, nf, ns, fsplit, kc, kf, chunks, period = cfg
    (
        trig_h, offs_h, coarse, fine, ctemp, ftemp, cweight, fweight, ctable, ftable,
        csnr, fout,
        trig, offs, coarse_v, fine_v, ctemp_v, ftemp_v, cw, fw, cstep, fstep,
        ag, outgoing, slots,
        cre0, cim0, cnre0, cre1, cim1, cnre1, fl0, fl1,
        cacc, cnorm, cnall, facc, fsum, fnorm, fnall, fsnr, back,
        crecv, frecv,
        in_sem, ct_sem, ft_sem,
        agr_send, agr_recv, agl_send, agl_recv, sl_send, sl_recv,
        cx_send, cx_recv, nx_send, nx_recv, fx_send, fx_recv, bk_send, bk_recv,
    ) = refs
    me = lax.axis_index("bank")
    fme = lax.axis_index("freq")
    sme = lax.axis_index("seg")
    seg_dev = coarse_v.shape[0]
    segs = nb * seg_dev
    rows = nb * CAP
    cbins = coarse_v.shape[2]
    fbins = fine_v.shape[2]
    csteps = cbins // kc
    fsteps = fbins // kf
    ctemps = ctemp_v.shape[1]
    sub_width = ftemp_v.shape[2]
    crow = ctemps // nf
    q = sub_width // nf
    fshare = q // fsplit
    nc = segs * LC
    nfl = rows * LF
    top_count = trig.shape[0]
    pairs = seg_dev * top_count
    cw_ag = cbins // chunks

    def win(i, width):
        return pl.ds(pl.multiple_of(i * width, width), width)

    small = [
        pltpu.make_async_copy(coarse, coarse_v, in_sem.at[0]),
        pltpu.make_async_copy(trig_h, trig, in_sem.at[6]),
        pltpu.make_async_copy(offs_h, offs, in_sem.at[7]),
        pltpu.make_async_copy(fine, fine_v, in_sem.at[1]),
        pltpu.make_async_copy(cweight, cw, in_sem.at[2]),
        pltpu.make_async_copy(fweight, fw, in_sem.at[3]),
        pltpu.make_async_copy(ctable.at[:, win(fme, cbins)], cstep, in_sem.at[4]),
        pltpu.make_async_copy(ftable.at[:, win(fme, fbins)], fstep, in_sem.at[5]),
    ]

    def ct_copy(i):
        return pltpu.make_async_copy(
            ctemp.at[:, :, win(i, kc)], ctemp_v.at[:, :, win(i, kc)], ct_sem.at[i]
        )

    def ft_copy(i):
        return pltpu.make_async_copy(
            ftemp.at[:, :, :, win(i, kf)], ftemp_v.at[:, :, :, win(i, kf)], ft_sem.at[i]
        )

    def ag_right(hop, chunk, block=None):
        block = me - hop if block is None else block
        view = ag.at[block, :, win(chunk, cw_ag)]
        return pltpu.make_async_remote_copy(
            src_ref=view, dst_ref=view,
            send_sem=agr_send.at[hop, chunk], recv_sem=agr_recv.at[hop, chunk],
            device_id={"bank": me + 1}, device_id_type=MESH,
        )

    def ag_left(hop, chunk, block=None):
        block = me + hop if block is None else block
        view = ag.at[block, :, win(chunk, cw_ag)]
        return pltpu.make_async_remote_copy(
            src_ref=view, dst_ref=view,
            send_sem=agl_send.at[hop, chunk], recv_sem=agl_recv.at[hop, chunk],
            device_id={"bank": me - 1}, device_id_type=MESH,
        )

    has_right = me + 1 < nb
    has_left = me >= 1

    def slot_copy(d, step):
        peer = lax.rem(me + d, nb)
        return pltpu.make_async_remote_copy(
            src_ref=outgoing.at[peer, :, win(step, kf)],
            dst_ref=slots.at[me, :, win(step, kf)],
            send_sem=sl_send.at[d - 1, step], recv_sem=sl_recv.at[d - 1, step],
            device_id={"bank": peer}, device_id_type=MESH,
        )

    def freq_copies(pairs_of, send, recv):
        copies = []
        for d in range(1, nf):
            peer = lax.rem(fme + d, nf)
            for k, (source, target) in enumerate(pairs_of):
                copies.append(
                    pltpu.make_async_remote_copy(
                        src_ref=source.at[peer], dst_ref=target.at[d - 1],
                        send_sem=send.at[d - 1, k], recv_sem=recv.at[d - 1, k],
                        device_id={"freq": peer}, device_id_type=MESH,
                    )
                )
        return copies

    def back_copies():
        return [
            pltpu.make_async_remote_copy(
                src_ref=fsnr, dst_ref=back.at[me],
                send_sem=bk_send.at[d - 1], recv_sem=bk_recv.at[d - 1],
                device_id={"bank": lax.rem(me + d, nb)}, device_id_type=MESH,
            )
            for d in range(1, nb)
        ]

    def by_part(block):
        block = block.astype(F32)
        return jnp.concatenate([block[:, 0, :], block[:, 1, :]], axis=0).astype(BF16)

    barrier = pltpu.get_barrier_semaphore()
    for d in range(1, nb):
        pl.semaphore_signal(
            barrier, inc=1, device_id={"bank": lax.rem(me + d, nb)}, device_id_type=MESH
        )
    for d in range(1, nf * ns):
        x, s = lax.rem(fme + d // ns, nf), lax.rem(sme + d % ns, ns)
        pl.semaphore_signal(
            barrier, inc=1, device_id={"freq": x, "seg": s}, device_id_type=MESH
        )
    for copy in small:
        copy.start()
    for i in range(csteps):
        ct_copy(i).start(priority=1)
        for k in range(i * fsteps // csteps, (i + 1) * fsteps // csteps):
            ft_copy(k).start(priority=1)
    small[0].wait()
    for c in range(chunks):
        ag[me, :, c * cw_ag : (c + 1) * cw_ag] = by_part(
            coarse_v[:, :, c * cw_ag : (c + 1) * cw_ag]
        )
    pl.semaphore_wait(barrier, nb - 1 + nf * ns - 1)
    for c in range(chunks):

        @pl.when(has_right)
        def _():
            ag_right(0, c).start()

        @pl.when(has_left)
        def _():
            ag_left(0, c).start()

    small[1].wait()
    own = [trig[p % top_count, me * seg_dev + p // top_count] for p in range(pairs)]

    def ranks_of(named):
        ranks = []
        for p in range(pairs):
            rank = jnp.int32(0)
            for before in range(p):
                rank = rank + (named[before] == named[p]).astype(I32)
            ranks.append(rank)
        return ranks

    own_rank = ranks_of(own)
    depth = 2 * CAP
    chooser_at = lax.broadcasted_iota(I32, (nb * depth, 2 * seg_dev), 0)
    chosen_col = jnp.zeros_like(chooser_at)
    for b in range(nb):
        for c in range(CAP):
            seg = jnp.int32(0)
            for p in range(pairs):
                hit = (own[p] == b) & (own_rank[p] == c)
                seg = jnp.where(hit, jnp.int32(p // top_count), seg)
            for part in range(2):
                chosen_col = jnp.where(
                    chooser_at == b * depth + part * CAP + c, seg + part * seg_dev, chosen_col
                )
    choice = jnp.where(
        lax.broadcasted_iota(I32, chooser_at.shape, 1) == chosen_col, 1.0, 0.0
    ).astype(BF16)

    small[3].wait()
    group = 2

    @pl.loop(0, fsteps // group)
    def _(i):
        for g in range(group):
            window = win(i * group + g, kf)
            chosen = jnp.dot(
                choice, by_part(fine_v[:, :, window]), preferred_element_type=F32
            ).astype(BF16)
            for b in range(nb):
                outgoing[b, :, window] = chosen[b * depth : (b + 1) * depth]

    slots[me] = outgoing[me]
    for copy in small[2:3] + small[4:]:
        copy.wait()

    cnorm[...] = jnp.zeros_like(cnorm)
    fnorm[...] = jnp.zeros_like(fnorm)
    cacc[...] = jnp.zeros_like(cacc)
    facc[...] = jnp.zeros_like(facc)

    cshare = crow // ns

    def norm_rows(acc, k, place, temps, start, bins, width, weight):
        part = None
        rows_at = pl.ds(pl.multiple_of(start, 16), 16)
        for c in range(0, width, 128):
            lanes = pl.ds(pl.multiple_of(bins + c, 128), 128)
            hr, hi = temps(rows_at, lanes)
            hr, hi = hr.astype(F32), hi.astype(F32)
            term = (hr * hr + hi * hi) * weight[:, c : c + 128]
            part = term if part is None else part + term
        acc[k, place : place + 16, :] += part

    def coarse_norm(i):
        ct_copy(i).wait()
        weight = cw[:, win(i, kc)]
        for k in range(nf):
            for r in range(0, cshare, 16):
                norm_rows(
                    cnorm, k, r,
                    lambda rows_at, lanes: (ctemp_v[0, rows_at, lanes], ctemp_v[1, rows_at, lanes]),
                    k * crow + sme * cshare + r, i * kc, kc, weight,
                )

    def fine_norm(i):
        ft_copy(i).wait()
        weight = fw[:, win(i, kf)]
        for k in range(nf):
            for r in range(0, fshare, 16):
                norm_rows(
                    fnorm, k, r,
                    lambda rows_at, lanes: (
                        ftemp_v[0, 0, rows_at, lanes], ftemp_v[1, 0, rows_at, lanes],
                    ),
                    k * q + (sme * fshare if fsplit > 1 else 0) + r, i * kf, kf, weight,
                )

    def slots_off(rightward):
        for dist in range(1, nb):
            there = me + dist < nb if rightward else me >= dist

            @pl.when(there)
            def _():
                @pl.loop(0, fsteps)
                def _(step):
                    slot_copy(dist if rightward else nb - dist, step).start()

    def gathered_chunk(hop, c):
        @pl.when(me - 1 - hop >= 0)
        def _():
            ag_right(hop, c, me - 1 - hop).wait_recv()

            @pl.when(has_right)
            def _():
                ag_right(hop + 1, c).start()

        @pl.when(me + 1 + hop < nb)
        def _():
            ag_left(hop, c, me + 1 + hop).wait_recv()

            @pl.when(has_left)
            def _():
                ag_left(hop + 1, c).start()

        if c == chunks - 1:

            @pl.when(me == hop + 1)
            def _():
                slots_off(True)

            @pl.when(nb - 1 - me == hop + 1)
            def _():
                slots_off(False)

    @pl.when(me == 0)
    def _():
        slots_off(True)

    @pl.when(me == nb - 1)
    def _():
        slots_off(False)

    events = [(hop, c) for hop in range(nb - 1) for c in range(chunks)]
    per = fsteps // csteps
    first = 2 * csteps // 8

    @pl.loop(0, csteps)
    def _(i):
        coarse_norm(i)
        for at in range(first, csteps):

            @pl.when(i == at)
            def _():
                gathered_chunk(*events[at - first])

        for k in range(per):
            fine_norm(i * per + k)

    cnall[fme, sme] = cnorm[fme]
    fnall[fme, sme if fsplit > 1 else 0] = fnorm[fme]
    norm_copies = []
    for dx in range(nf):
        for ds in range(ns):
            if dx + ds == 0:
                continue
            x, s = lax.rem(fme + dx, nf), lax.rem(sme + ds, ns)
            kinds = [(cnorm, cnall, sme)]
            if fsplit > 1 or ds == 0:
                kinds.append((fnorm, fnall, sme if fsplit > 1 else 0))
            for kind, (source, target, at) in enumerate(kinds):
                norm_copies.append(
                    pltpu.make_async_remote_copy(
                        src_ref=source.at[x], dst_ref=target.at[fme, at],
                        send_sem=nx_send.at[dx * ns + ds, kind],
                        recv_sem=nx_recv.at[dx * ns + ds, kind],
                        device_id={"freq": x, "seg": s}, device_id_type=MESH,
                    )
                )
    for copy in norm_copies:
        copy.start()
    for event in events[csteps - first :]:
        gathered_chunk(*event)

    cbuf = ((cre0, cim0, cnre0), (cre1, cim1, cnre1))

    def coarse_lags(i, buf):
        re_ref, im_ref, nre_ref = buf
        sub = 256
        for c in range(0, kc, sub):
            window = pl.ds(pl.multiple_of(i * kc + c, sub), sub)
            blocks = [ag[b, :, window].astype(F32) for b in range(nb)]
            w = cw[:, window]
            real = jnp.concatenate([x[:seg_dev] for x in blocks], axis=0) * w
            imag = jnp.concatenate([x[seg_dev:] for x in blocks], axis=0) * w

            def emit(j, re, im):
                re = re.astype(BF16)
                re_ref[j * segs : (j + 1) * segs, c : c + sub] = re
                nre_ref[j * segs : (j + 1) * segs, c : c + sub] = -re
                im_ref[j * segs : (j + 1) * segs, c : c + sub] = im.astype(BF16)

            lag_series(real, imag, cstep[0:1, window], cstep[1:2, window], LC, emit)

    def coarse_products(i, buf):
        re_ref, im_ref, nre_ref = buf
        window = win(i, kc)
        left = jnp.concatenate([ctemp_v[0, :, window], ctemp_v[1, :, window]], axis=1)
        re, im, nre = re_ref[...], im_ref[...], nre_ref[...]
        right = jnp.concatenate(
            [jnp.concatenate([re, im], axis=1), jnp.concatenate([im, nre], axis=1)], axis=0
        )
        out = nt_dot(left, right)
        for k in range(nf):
            cacc[k] += out[k * crow : (k + 1) * crow]

    coarse_lags(0, cbuf[0])

    @pl.loop(0, csteps // 2)
    def _(i):
        coarse_lags(2 * i + 1, cbuf[1])
        coarse_products(2 * i, cbuf[0])
        coarse_lags(jnp.minimum(2 * i + 2, csteps - 1), cbuf[0])
        coarse_products(2 * i + 1, cbuf[1])

    coarse_copies = freq_copies(((cacc, crecv),), cx_send, cx_recv)
    for copy in coarse_copies:
        copy.start()

    row_at = lax.broadcasted_iota(I32, (rows, 128), 0)
    shift = jnp.zeros((rows, 128), I32)
    for b in range(nb):
        block = [trig[p % top_count, b * seg_dev + p // top_count] for p in range(pairs)]
        taken = jnp.int32(0)
        for p in range(pairs):
            hit = block[p] == me
            offset = offs[p % top_count, b * seg_dev + p // top_count]
            shift = jnp.where(
                row_at == jnp.where(hit, b * CAP + taken, -1), offset, shift
            )
            taken = taken + hit.astype(I32)
    lane = lax.broadcasted_iota(I32, (rows, 128), 1)
    tiles = fbins // 128
    lane_angle = ((shift * lane) & (period - 1)).astype(F32) * (2.0 * math.pi / period)
    lane_cos, lane_sin = jnp.cos(lane_angle), jnp.sin(lane_angle)
    coarse_period = period // 128
    tile_at = lax.broadcasted_iota(I32, (rows, tiles), 1) + fme * tiles
    wide = jnp.concatenate([shift] * (tiles // 128), axis=1)
    tile_angle = ((wide * tile_at) & (coarse_period - 1)).astype(F32) * (
        2.0 * math.pi / coarse_period
    )
    tile_cos, tile_sin = jnp.cos(tile_angle), jnp.sin(tile_angle)

    def fine_lags(i, buf):
        per = kf // 128
        turn = lax.rem(tiles - i * per, tiles)
        here_cos = pltpu.roll(tile_cos, turn, 1)
        here_sin = pltpu.roll(tile_sin, turn, 1)
        sub = 512
        for c in range(0, kf, sub):
            window = pl.ds(pl.multiple_of(i * kf + c, sub), sub)
            blocks = [slots[b, :, window].astype(F32) for b in range(nb)]
            w = fw[:, window]
            real = jnp.concatenate([x[:CAP] for x in blocks], axis=0) * w
            imag = jnp.concatenate([x[CAP:] for x in blocks], axis=0) * w
            turn_re, turn_im = [], []
            for t in range(c // 128, (c + sub) // 128):
                a_cos = here_cos[:, t : t + 1]
                a_sin = here_sin[:, t : t + 1]
                turn_re.append(a_cos * lane_cos - a_sin * lane_sin)
                turn_im.append(a_cos * lane_sin + a_sin * lane_cos)
            sr = jnp.concatenate(turn_re, axis=1)
            si = jnp.concatenate(turn_im, axis=1)
            real, imag = real * sr - imag * si, real * si + imag * sr
            held = []

            def emit(j, re, im):
                held.append((re, im))
                if len(held) == 2:
                    low, high = (j - 1) * rows, (j + 1) * rows
                    buf[low:high, c : c + sub] = jnp.concatenate(
                        [held[0][0], held[1][0]], axis=0
                    ).astype(BF16)
                    buf[nfl + low : nfl + high, c : c + sub] = jnp.concatenate(
                        [held[0][1], held[1][1]], axis=0
                    ).astype(BF16)
                    held.clear()

            lag_series(real, imag, fstep[0:1, window], fstep[1:2, window], LF, emit)

    def fine_products(i, buf):
        window = win(i, kf)
        left = jnp.concatenate([ftemp_v[0, 0, :, window], ftemp_v[1, 0, :, window]], axis=0)
        facc[...] += nt_dot(left, buf[...])

    def slots_here(step):
        for d in range(1, nb):
            slot_copy(d, step).wait_recv()

    slots_here(0)
    fine_lags(0, fl0)

    @pl.loop(0, fsteps // 2 - 1)
    def _(i):
        slots_here(2 * i + 1)
        slots_here(2 * i + 2)
        fine_lags(2 * i + 1, fl1)
        fine_products(2 * i, fl0)
        fine_lags(2 * i + 2, fl0)
        fine_products(2 * i + 1, fl1)

    slots_here(fsteps - 1)
    fine_lags(fsteps - 1, fl1)
    fine_products(fsteps - 2, fl0)
    fine_products(fsteps - 1, fl1)

    both = facc.shape[0] // 2
    re = facc[:both, :nfl] + facc[both:, nfl:]
    im = facc[:both, nfl:] - facc[both:, :nfl]
    for k in range(nf):
        fsum[k, 0] = re[k * q : (k + 1) * q]
        fsum[k, 1] = im[k * q : (k + 1) * q]
    fine_copies = freq_copies(((fsum, frecv),), fx_send, fx_recv)
    for copy in fine_copies:
        copy.start()
    for copy in norm_copies + fine_copies:
        copy.wait_recv()
    def whole_norm(parts):
        shares = []
        for s in range(parts.shape[1]):
            total = parts[0, s]
            for x in range(1, nf):
                total = total + parts[x, s]
            shares.append(total)
        return jnp.sum(jnp.concatenate(shares, axis=0), axis=1, keepdims=True)

    re, im = fsum[fme, 0], fsum[fme, 1]
    for d in range(nf - 1):
        re = re + frecv[d, 0]
        im = im + frecv[d, 1]
    top = peak(re * re + im * im, rows)[:, :128]
    fsnr[...] = top / whole_norm(fnall)
    bcopies = back_copies()
    for copy in bcopies:
        copy.start()
    back[me] = fsnr[...]

    for copy in coarse_copies:
        copy.wait_recv()
    acc = cacc[fme]
    for d in range(nf - 1):
        acc = acc + crecv[d]
    re, im = acc[:, :nc], acc[:, nc:]
    top = peak(re * re + im * im, segs)
    csnr[...] = jnp.transpose(top[:, :128] / whole_norm(cnall))[:segs]

    for copy in coarse_copies + norm_copies + fine_copies:
        copy.wait_send()
    for hop in range(nb - 1):
        for c in range(chunks):

            @pl.when(has_right & (me - hop >= 0))
            def _():
                ag_right(hop, c).wait_send()

            @pl.when(has_left & (me + hop < nb))
            def _():
                ag_left(hop, c).wait_send()

    @pl.loop(0, fsteps)
    def _(step):
        for d in range(1, nb):
            slot_copy(d, step).wait_send()

    for copy in bcopies:
        copy.wait()
    at = lax.broadcasted_iota(I32, back.shape[1:], 1)
    gathered = jnp.zeros(back.shape[1:], F32)
    for b in range(nb):
        turned = pltpu.roll(back[b], lax.rem((b - me + nb) * CAP + 128 - nb * CAP, 128), 1)
        gathered = jnp.where((at >= b * CAP) & (at < (b + 1) * CAP), turned, gathered)
    pair_at = lax.broadcasted_iota(I32, (pairs, 128), 0)
    place = jnp.zeros((pairs, 128), I32)
    for p in range(pairs):
        place = jnp.where(pair_at == p, own[p] * CAP + own_rank[p], place)
    giver = jnp.where(lax.broadcasted_iota(I32, (pairs, 128), 1) == place, 1.0, 0.0)
    fout[...] = lax.dot_general(
        giver, gathered, (((1,), (1,)), ((), ())),
        precision=lax.Precision.HIGHEST, preferred_element_type=F32,
    )


def body(
    coarse_spectra,
    fine_spectra,
    coarse_templates,
    fine_templates,
    coarse_weight,
    fine_weight,
    triggers,
    offsets,
):
    nb = lax.axis_size("bank")
    nf = lax.axis_size("freq")
    ns = lax.axis_size("seg")
    seg_local = fine_spectra.shape[0]
    cbins = coarse_spectra.shape[2]
    fbins = fine_spectra.shape[2]
    top_count = triggers.shape[1]
    sub_width = fine_templates.shape[2]
    ctemps = coarse_templates.shape[1]
    rows = nb * CAP
    segs = nb * seg_local
    kc = min(1024, cbins // 2)
    kf = min(2048, fbins // 2)
    chunks = 4
    csteps = cbins // kc
    fsteps = fbins // kf
    crow = ctemps // nf
    q = sub_width // nf
    period = 2 * fbins * nf
    fsplit = ns if q // ns % 16 == 0 else 1
    assert period & (period - 1) == 0 and csteps % 2 == 0 and fsteps % 2 == 0
    nc = segs * LC
    nfl = rows * LF
    ctable = jnp.asarray(unit_table(cbins * nf, CSTRIDE, 2 * cbins * nf))
    ftable = jnp.asarray(unit_table(fbins * nf, 1, period))

    vmem, anywhere = pl.BlockSpec(memory_space=pltpu.VMEM), pl.BlockSpec(memory_space=pl.ANY)
    dma = pltpu.SemaphoreType.DMA
    lag_buf = pltpu.VMEM((nc, kc), BF16)
    fine_buf = pltpu.VMEM((2 * nfl, kf), BF16)
    csnr, fine_rows = pl.pallas_call(
        functools.partial(kernel, (nb, nf, ns, fsplit, kc, kf, chunks, period)),
        out_shape=(
            jax.ShapeDtypeStruct((segs, crow), F32),
            jax.ShapeDtypeStruct((seg_local * top_count, q), F32),
        ),
        in_specs=[anywhere] * 10,
        out_specs=(vmem, vmem),
        scratch_shapes=[
            pltpu.SMEM((top_count, triggers.shape[0]), I32),
            pltpu.SMEM((top_count, triggers.shape[0]), I32),
            pltpu.VMEM(coarse_spectra.shape, BF16),
            pltpu.VMEM(fine_spectra.shape, BF16),
            pltpu.VMEM(coarse_templates.shape, BF16),
            pltpu.VMEM(fine_templates.shape, BF16),
            pltpu.VMEM((1, cbins), F32),
            pltpu.VMEM((1, fbins), F32),
            pltpu.VMEM((2, cbins), F32),
            pltpu.VMEM((2, fbins), F32),
            pltpu.VMEM((nb, 2 * seg_local, cbins), BF16),
            pltpu.VMEM((nb, 2 * CAP, fbins), BF16),
            pltpu.VMEM((nb, 2 * CAP, fbins), BF16),
            lag_buf, lag_buf, lag_buf, lag_buf, lag_buf, lag_buf,
            fine_buf, fine_buf,
            pltpu.VMEM((nf, crow, 2 * nc), F32),
            pltpu.VMEM((nf, crow // ns, 128), F32),
            pltpu.VMEM((nf, ns, crow // ns, 128), F32),
            pltpu.VMEM((2 * sub_width, 2 * nfl), F32),
            pltpu.VMEM((nf, 2, q, nfl), F32),
            pltpu.VMEM((nf, q // fsplit, 128), F32),
            pltpu.VMEM((nf, fsplit, q // fsplit, 128), F32),
            pltpu.VMEM((q, 128), F32),
            pltpu.VMEM((nb, q, 128), F32),
            pltpu.VMEM((nf - 1, crow, 2 * nc), F32),
            pltpu.VMEM((nf - 1, 2, q, nfl), F32),
            dma((8,)),
            dma((csteps,)),
            dma((fsteps,)),
            dma((nb - 1, chunks)),
            dma((nb - 1, chunks)),
            dma((nb - 1, chunks)),
            dma((nb - 1, chunks)),
            dma((nb - 1, fsteps)),
            dma((nb - 1, fsteps)),
            dma((nf - 1, 1)),
            dma((nf - 1, 1)),
            dma((nf * ns, 2)),
            dma((nf * ns, 2)),
            dma((nf - 1, 1)),
            dma((nf - 1, 1)),
            dma((nb - 1,)),
            dma((nb - 1,)),
        ],
        compiler_params=pltpu.CompilerParams(
            collective_id=0,
            has_side_effects=True,
            vmem_limit_bytes=60 * 1024 * 1024,
        ),
    )(
        triggers.T,
        offsets.T,
        coarse_spectra,
        fine_spectra,
        coarse_templates,
        fine_templates,
        coarse_weight[None, :],
        fine_weight[None, :],
        ctable,
        ftable,
    )
    return (csnr.T, fine_rows.reshape(seg_local, top_count, q))


def solution(mesh):
    return jax.shard_map(
        body,
        mesh=mesh,
        in_specs=(
            P(("groups", "seg", "bank"), None, "freq"),
            P(("groups", "seg", "bank"), None, "freq"),
            P(None, "bank", "freq"),
            P(None, "bank", None, "freq"),
            P(("groups", "freq")),
            P(("groups", "freq")),
            P(("groups", "seg"), None),
            P(("groups", "seg"), None),
        ),
        out_specs=(
            P(("bank", "freq"), ("groups", "seg")),
            P(("groups", "seg", "bank"), None, "freq"),
        ),
        check_vma=False,
    )
```

```python
import functools
import math

import jax
import jax.numpy as jnp
import numpy as np
from jax import lax
from jax.experimental import pallas as pl
from jax.experimental.pallas import tpu as pltpu
from jax.sharding import PartitionSpec as P

CAP = 2
LC = 16
LF = 16
CSTRIDE = 2047

MESH = pl.DeviceIdType.MESH
F32 = jnp.float32
BF16 = jnp.bfloat16
I32 = jnp.int32


def unit_table(count, stride, period):
    angle = 2.0 * np.pi * ((np.arange(count) * stride) % period) / period
    return np.stack([np.cos(angle), np.sin(angle)]).astype(np.float32)


def nt_dot(left, right):
    return lax.dot_general(left, right, (((1,), (1,)), ((), ())), preferred_element_type=F32)


def lag_series(real, imag, cos, sin, lags, emit):
    emit(0, real, imag)
    prev_re, prev_im = real, imag
    real, imag = real * cos - imag * sin, real * sin + imag * cos
    twice = cos + cos
    for j in range(1, lags):
        emit(j, real, imag)
        if j + 1 < lags:
            next_re = twice * real - prev_re
            next_im = twice * imag - prev_im
            prev_re, prev_im, real, imag = real, imag, next_re, next_im


def peak(energy, width):
    total = energy.shape[1]
    while total > width:
        half = total // 2
        if half % 128 == 0:
            energy = jnp.maximum(energy[:, :half], energy[:, half:])
        else:
            energy = jnp.maximum(energy, pltpu.roll(energy, energy.shape[1] - half, 1))
        total = half
    return energy


def kernel(cfg, *refs):
    nb, nf, ns, fsplit, kc, kf, chunks, period = cfg
    (
        trig_h, offs_h, coarse, fine, ctemp, ftemp, cweight, fweight, ctable, ftable,
        csnr, fout,
        trig, offs, coarse_v, fine_v, ctemp_v, ftemp_v, cw, fw, cstep, fstep,
        ag, outgoing, slots,
        cre0, cim0, cnre0, cre1, cim1, cnre1, fl0, fl1,
        cacc, cnorm, cnall, facc, fsum, fnorm, fnall, fsnr, back,
        csend, crecv, frecv,
        in_sem, ct_sem, ft_sem,
        agr_send, agr_recv, agl_send, agl_recv, sl_send, sl_recv,
        cx_send, cx_recv, nx_send, nx_recv, fx_send, fx_recv, bk_send, bk_recv,
    ) = refs
    me = lax.axis_index("bank")
    fme = lax.axis_index("freq")
    sme = lax.axis_index("seg")
    seg_dev = coarse_v.shape[0]
    segs = nb * seg_dev
    rows = nb * CAP
    cbins = coarse_v.shape[2]
    fbins = fine_v.shape[2]
    csteps = cbins // kc
    fsteps = fbins // kf
    ctemps = ctemp_v.shape[1]
    sub_width = ftemp_v.shape[2]
    crow = ctemps // nf
    q = sub_width // nf
    fshare = q // fsplit
    nc = segs * LC
    nfl = rows * LF
    top_count = trig.shape[0]
    pairs = seg_dev * top_count
    cw_ag = cbins // chunks

    def win(i, width):
        return pl.ds(pl.multiple_of(i * width, width), width)

    small = [
        pltpu.make_async_copy(coarse, coarse_v, in_sem.at[0]),
        pltpu.make_async_copy(trig_h, trig, in_sem.at[6]),
        pltpu.make_async_copy(offs_h, offs, in_sem.at[7]),
        pltpu.make_async_copy(fine, fine_v, in_sem.at[1]),
        pltpu.make_async_copy(cweight, cw, in_sem.at[2]),
        pltpu.make_async_copy(fweight, fw, in_sem.at[3]),
        pltpu.make_async_copy(ctable.at[:, win(fme, cbins)], cstep, in_sem.at[4]),
        pltpu.make_async_copy(ftable.at[:, win(fme, fbins)], fstep, in_sem.at[5]),
    ]

    def ct_copy(i):
        return pltpu.make_async_copy(
            ctemp.at[:, :, win(i, kc)], ctemp_v.at[:, :, win(i, kc)], ct_sem.at[i]
        )

    def ft_copy(i):
        return pltpu.make_async_copy(
            ftemp.at[:, :, :, win(i, kf)], ftemp_v.at[:, :, :, win(i, kf)], ft_sem.at[i]
        )

    def ag_right(hop, chunk, block=None):
        block = me - hop if block is None else block
        view = ag.at[block, :, win(chunk, cw_ag)]
        return pltpu.make_async_remote_copy(
            src_ref=view, dst_ref=view,
            send_sem=agr_send.at[hop, chunk], recv_sem=agr_recv.at[hop, chunk],
            device_id={"bank": me + 1}, device_id_type=MESH,
        )

    def ag_left(hop, chunk, block=None):
        block = me + hop if block is None else block
        view = ag.at[block, :, win(chunk, cw_ag)]
        return pltpu.make_async_remote_copy(
            src_ref=view, dst_ref=view,
            send_sem=agl_send.at[hop, chunk], recv_sem=agl_recv.at[hop, chunk],
            device_id={"bank": me - 1}, device_id_type=MESH,
        )

    has_right = me + 1 < nb
    has_left = me >= 1

    couples = fsteps // 2 - 1

    def slot_copy(d, place, start, width):
        peer = lax.rem(me + d, nb)
        window = pl.ds(pl.multiple_of(start, kf), width)
        return pltpu.make_async_remote_copy(
            src_ref=outgoing.at[peer, :, window],
            dst_ref=slots.at[me, :, window],
            send_sem=sl_send.at[d - 1, place], recv_sem=sl_recv.at[d - 1, place],
            device_id={"bank": peer}, device_id_type=MESH,
        )

    def slot_couple(d, g):
        return slot_copy(d, g, g * 2 * kf, 2 * kf)

    def slot_last(d, k):
        return slot_copy(d, couples + k, (2 * couples + k) * kf, kf)

    def freq_copies(pairs_of, send, recv):
        copies = []
        for d in range(1, nf):
            peer = lax.rem(fme + d, nf)
            for k, (source, target) in enumerate(pairs_of):
                copies.append(
                    pltpu.make_async_remote_copy(
                        src_ref=source.at[peer], dst_ref=target.at[d - 1],
                        send_sem=send.at[d - 1, k], recv_sem=recv.at[d - 1, k],
                        device_id={"freq": peer}, device_id_type=MESH,
                    )
                )
        return copies

    def back_copies():
        return [
            pltpu.make_async_remote_copy(
                src_ref=fsnr, dst_ref=back.at[me],
                send_sem=bk_send.at[d - 1], recv_sem=bk_recv.at[d - 1],
                device_id={"bank": lax.rem(me + d, nb)}, device_id_type=MESH,
            )
            for d in range(1, nb)
        ]

    def by_part(block):
        block = block.astype(F32)
        return jnp.concatenate([block[:, 0, :], block[:, 1, :]], axis=0).astype(BF16)

    barrier = pltpu.get_barrier_semaphore()
    for d in range(1, nb):
        pl.semaphore_signal(
            barrier, inc=1, device_id={"bank": lax.rem(me + d, nb)}, device_id_type=MESH
        )
    for d in range(1, nf * ns):
        x, s = lax.rem(fme + d // ns, nf), lax.rem(sme + d % ns, ns)
        pl.semaphore_signal(
            barrier, inc=1, device_id={"freq": x, "seg": s}, device_id_type=MESH
        )
    for copy in small:
        copy.start()
    for i in range(csteps):
        ct_copy(i).start(priority=1)
        for k in range(i * fsteps // csteps, (i + 1) * fsteps // csteps):
            ft_copy(k).start(priority=1)
    small[0].wait()
    for c in range(chunks):
        ag[me, :, c * cw_ag : (c + 1) * cw_ag] = by_part(
            coarse_v[:, :, c * cw_ag : (c + 1) * cw_ag]
        )
    pl.semaphore_wait(barrier, nb - 1 + nf * ns - 1)
    for c in range(chunks):

        @pl.when(has_right)
        def _():
            ag_right(0, c).start()

        @pl.when(has_left)
        def _():
            ag_left(0, c).start()

    small[1].wait()
    own = [trig[p % top_count, me * seg_dev + p // top_count] for p in range(pairs)]

    def ranks_of(named):
        ranks = []
        for p in range(pairs):
            rank = jnp.int32(0)
            for before in range(p):
                rank = rank + (named[before] == named[p]).astype(I32)
            ranks.append(rank)
        return ranks

    own_rank = ranks_of(own)
    depth = 2 * CAP
    chooser_at = lax.broadcasted_iota(I32, (nb * depth, 2 * seg_dev), 0)
    chosen_col = jnp.zeros_like(chooser_at)
    for b in range(nb):
        for c in range(CAP):
            seg = jnp.int32(0)
            for p in range(pairs):
                hit = (own[p] == b) & (own_rank[p] == c)
                seg = jnp.where(hit, jnp.int32(p // top_count), seg)
            for part in range(2):
                chosen_col = jnp.where(
                    chooser_at == b * depth + part * CAP + c, seg + part * seg_dev, chosen_col
                )
    choice = jnp.where(
        lax.broadcasted_iota(I32, chooser_at.shape, 1) == chosen_col, 1.0, 0.0
    ).astype(BF16)

    small[3].wait()
    group = 2

    @pl.loop(0, fsteps // group)
    def _(i):
        for g in range(group):
            window = win(i * group + g, kf)
            chosen = jnp.dot(
                choice, by_part(fine_v[:, :, window]), preferred_element_type=F32
            ).astype(BF16)
            for b in range(nb):
                outgoing[b, :, window] = chosen[b * depth : (b + 1) * depth]

    slots[me] = outgoing[me]
    for copy in small[2:3] + small[4:]:
        copy.wait()

    cnorm[...] = jnp.zeros_like(cnorm)
    fnorm[...] = jnp.zeros_like(fnorm)
    cacc[...] = jnp.zeros_like(cacc)
    facc[...] = jnp.zeros_like(facc)

    cshare = crow // ns

    def norm_rows(acc, k, place, temps, start, bins, width, weight):
        part = None
        rows_at = pl.ds(pl.multiple_of(start, 16), 16)
        for c in range(0, width, 128):
            lanes = pl.ds(pl.multiple_of(bins + c, 128), 128)
            hr, hi = temps(rows_at, lanes)
            hr, hi = hr.astype(F32), hi.astype(F32)
            term = (hr * hr + hi * hi) * weight[:, c : c + 128]
            part = term if part is None else part + term
        acc[k, place : place + 16, :] += part

    def coarse_norm(i):
        ct_copy(i).wait()
        weight = cw[:, win(i, kc)]
        for k in range(nf):
            for r in range(0, cshare, 16):
                norm_rows(
                    cnorm, k, r,
                    lambda rows_at, lanes: (ctemp_v[0, rows_at, lanes], ctemp_v[1, rows_at, lanes]),
                    k * crow + sme * cshare + r, i * kc, kc, weight,
                )

    def fine_norm(i):
        ft_copy(i).wait()
        weight = fw[:, win(i, kf)]
        for k in range(nf):
            for r in range(0, fshare, 16):
                norm_rows(
                    fnorm, k, r,
                    lambda rows_at, lanes: (
                        ftemp_v[0, 0, rows_at, lanes], ftemp_v[1, 0, rows_at, lanes],
                    ),
                    k * q + (sme * fshare if fsplit > 1 else 0) + r, i * kf, kf, weight,
                )

    def send_slots(rightward, dists, low, high):
        def send(dist, copy):
            there = me + dist < nb if rightward else me >= dist

            @pl.when(there)
            def _():
                copy(dist if rightward else nb - dist).start()

        @pl.loop(low, min(high, couples))
        def _(g):
            for dist in dists:
                send(dist, lambda d: slot_couple(d, g))

        if high > couples:
            for k in range(2):
                for dist in dists:
                    send(dist, lambda d: slot_last(d, k))

    def slots_off(rightward, end):
        if end:
            send_slots(rightward, [1], 0, couples + 1)
            send_slots(rightward, range(2, nb), 0, couples + 1)
        else:
            send_slots(rightward, range(1, nb), 1, couples + 1)

    @pl.when(me > 0)
    def _():
        send_slots(True, range(1, nb), 0, 1)

    @pl.when(me < nb - 1)
    def _():
        send_slots(False, range(1, nb), 0, 1)

    def gathered_chunk(hop, c):
        @pl.when(me - 1 - hop >= 0)
        def _():
            ag_right(hop, c, me - 1 - hop).wait_recv()

            @pl.when(has_right)
            def _():
                ag_right(hop + 1, c).start()

        @pl.when(me + 1 + hop < nb)
        def _():
            ag_left(hop, c, me + 1 + hop).wait_recv()

            @pl.when(has_left)
            def _():
                ag_left(hop + 1, c).start()

        if c == chunks - 1:

            @pl.when(me == hop + 1)
            def _():
                slots_off(True, False)

            @pl.when(nb - 1 - me == hop + 1)
            def _():
                slots_off(False, False)

    @pl.when(me == 0)
    def _():
        slots_off(True, True)

    @pl.when(me == nb - 1)
    def _():
        slots_off(False, True)

    events = [(hop, c) for hop in range(nb - 2) for c in range(chunks)]
    per = fsteps // csteps
    first = 2 * csteps // 8

    @pl.loop(0, csteps)
    def _(i):
        coarse_norm(i)
        for at in range(first, csteps):

            @pl.when(i == at)
            def _():
                gathered_chunk(*events[at - first])

        for k in range(per):
            fine_norm(i * per + k)

    cnall[fme, sme] = cnorm[fme]
    fnall[fme, sme if fsplit > 1 else 0] = fnorm[fme]
    norm_copies = []
    for dx in range(nf):
        for ds in range(ns):
            if dx + ds == 0:
                continue
            x, s = lax.rem(fme + dx, nf), lax.rem(sme + ds, ns)
            kinds = [(cnorm, cnall, sme)]
            if fsplit > 1 or ds == 0:
                kinds.append((fnorm, fnall, sme if fsplit > 1 else 0))
            for kind, (source, target, at) in enumerate(kinds):
                norm_copies.append(
                    pltpu.make_async_remote_copy(
                        src_ref=source.at[x], dst_ref=target.at[fme, at],
                        send_sem=nx_send.at[dx * ns + ds, kind],
                        recv_sem=nx_recv.at[dx * ns + ds, kind],
                        device_id={"freq": x, "seg": s}, device_id_type=MESH,
                    )
                )
    for copy in norm_copies:
        copy.start()
    for event in events[csteps - first :]:
        gathered_chunk(*event)

    cbuf = ((cre0, cim0, cnre0), (cre1, cim1, cnre1))

    def coarse_lags(i, buf):
        re_ref, im_ref, nre_ref = buf
        sub = 256
        for c in range(0, kc, sub):
            window = pl.ds(pl.multiple_of(i * kc + c, sub), sub)
            blocks = [ag[b, :, window].astype(F32) for b in range(nb)]
            w = cw[:, window]
            real = jnp.concatenate([x[:seg_dev] for x in blocks], axis=0) * w
            imag = jnp.concatenate([x[seg_dev:] for x in blocks], axis=0) * w

            def emit(j, re, im):
                re = re.astype(BF16)
                re_ref[j * segs : (j + 1) * segs, c : c + sub] = re
                nre_ref[j * segs : (j + 1) * segs, c : c + sub] = -re
                im_ref[j * segs : (j + 1) * segs, c : c + sub] = im.astype(BF16)

            lag_series(real, imag, cstep[0:1, window], cstep[1:2, window], LC, emit)

    def coarse_products(i, buf):
        re_ref, im_ref, nre_ref = buf
        window = win(i, kc)
        left = jnp.concatenate([ctemp_v[0, :, window], ctemp_v[1, :, window]], axis=1)
        re, im, nre = re_ref[...], im_ref[...], nre_ref[...]
        right = jnp.concatenate(
            [jnp.concatenate([re, im], axis=1), jnp.concatenate([im, nre], axis=1)], axis=0
        )
        out = nt_dot(left, right)
        for k in range(nf):
            cacc[k] += out[k * crow : (k + 1) * crow]

    def last_hop(c):
        @pl.when(me == nb - 1)
        def _():
            ag_right(nb - 2, c, 0).wait_recv()

        @pl.when(me == 0)
        def _():
            ag_left(nb - 2, c, nb - 1).wait_recv()

    last_hop(0)
    coarse_lags(0, cbuf[0])

    @pl.loop(0, csteps // 2)
    def _(i):
        @pl.when(i + 1 < chunks)
        def _():
            last_hop(i + 1)

        coarse_lags(2 * i + 1, cbuf[1])
        coarse_products(2 * i, cbuf[0])
        coarse_lags(jnp.minimum(2 * i + 2, csteps - 1), cbuf[0])
        coarse_products(2 * i + 1, cbuf[1])

    for d in range(1, nf):
        peer = lax.rem(fme + d, nf)
        csend[peer] = cacc[peer].astype(BF16)
    coarse_copies = freq_copies(((csend, crecv),), cx_send, cx_recv)
    for copy in coarse_copies:
        copy.start()

    row_at = lax.broadcasted_iota(I32, (rows, 128), 0)
    shift = jnp.zeros((rows, 128), I32)
    for b in range(nb):
        block = [trig[p % top_count, b * seg_dev + p // top_count] for p in range(pairs)]
        taken = jnp.int32(0)
        for p in range(pairs):
            hit = block[p] == me
            offset = offs[p % top_count, b * seg_dev + p // top_count]
            shift = jnp.where(
                row_at == jnp.where(hit, b * CAP + taken, -1), offset, shift
            )
            taken = taken + hit.astype(I32)
    lane = lax.broadcasted_iota(I32, (rows, 128), 1)
    tiles = fbins // 128
    lane_angle = ((shift * lane) & (period - 1)).astype(F32) * (2.0 * math.pi / period)
    lane_cos, lane_sin = jnp.cos(lane_angle), jnp.sin(lane_angle)
    coarse_period = period // 128
    tile_at = lax.broadcasted_iota(I32, (rows, tiles), 1) + fme * tiles
    wide = jnp.concatenate([shift] * (tiles // 128), axis=1)
    tile_angle = ((wide * tile_at) & (coarse_period - 1)).astype(F32) * (
        2.0 * math.pi / coarse_period
    )
    tile_cos, tile_sin = jnp.cos(tile_angle), jnp.sin(tile_angle)

    def fine_lags(i, buf):
        per = kf // 128
        turn = lax.rem(tiles - i * per, tiles)
        here_cos = pltpu.roll(tile_cos, turn, 1)
        here_sin = pltpu.roll(tile_sin, turn, 1)
        sub = 512
        for c in range(0, kf, sub):
            window = pl.ds(pl.multiple_of(i * kf + c, sub), sub)
            blocks = [slots[b, :, window].astype(F32) for b in range(nb)]
            w = fw[:, window]
            real = jnp.concatenate([x[:CAP] for x in blocks], axis=0) * w
            imag = jnp.concatenate([x[CAP:] for x in blocks], axis=0) * w
            turn_re, turn_im = [], []
            for t in range(c // 128, (c + sub) // 128):
                a_cos = here_cos[:, t : t + 1]
                a_sin = here_sin[:, t : t + 1]
                turn_re.append(a_cos * lane_cos - a_sin * lane_sin)
                turn_im.append(a_cos * lane_sin + a_sin * lane_cos)
            sr = jnp.concatenate(turn_re, axis=1)
            si = jnp.concatenate(turn_im, axis=1)
            real, imag = real * sr - imag * si, real * si + imag * sr
            held = []

            def emit(j, re, im):
                held.append((re, im))
                if len(held) == 2:
                    low, high = (j - 1) * rows, (j + 1) * rows
                    buf[low:high, c : c + sub] = jnp.concatenate(
                        [held[0][0], held[1][0]], axis=0
                    ).astype(BF16)
                    buf[nfl + low : nfl + high, c : c + sub] = jnp.concatenate(
                        [held[0][1], held[1][1]], axis=0
                    ).astype(BF16)
                    held.clear()

            lag_series(real, imag, fstep[0:1, window], fstep[1:2, window], LF, emit)

    def fine_products(i, buf):
        window = win(i, kf)
        left = jnp.concatenate([ftemp_v[0, 0, :, window], ftemp_v[1, 0, :, window]], axis=0)
        facc[...] += nt_dot(left, buf[...])

    def slots_here(copy, at):
        for d in range(1, nb):
            copy(d, at).wait_recv()

    slots_here(slot_couple, 0)
    fine_lags(0, fl0)

    @pl.loop(0, fsteps // 2 - 1)
    def _(i):
        @pl.when(i + 1 < couples)
        def _():
            slots_here(slot_couple, i + 1)

        @pl.when(i + 1 == couples)
        def _():
            slots_here(slot_last, 0)

        fine_lags(2 * i + 1, fl1)
        fine_products(2 * i, fl0)
        fine_lags(2 * i + 2, fl0)
        fine_products(2 * i + 1, fl1)

    slots_here(slot_last, 1)
    fine_lags(fsteps - 1, fl1)
    fine_products(fsteps - 2, fl0)
    fine_products(fsteps - 1, fl1)

    both = facc.shape[0] // 2
    re = facc[:both, :nfl] + facc[both:, nfl:]
    im = facc[:both, nfl:] - facc[both:, :nfl]
    for k in range(nf):
        fsum[k, 0] = re[k * q : (k + 1) * q]
        fsum[k, 1] = im[k * q : (k + 1) * q]
    fine_copies = freq_copies(((fsum, frecv),), fx_send, fx_recv)
    for copy in fine_copies:
        copy.start()
    for copy in norm_copies + fine_copies:
        copy.wait_recv()
    def whole_norm(parts):
        shares = []
        for s in range(parts.shape[1]):
            total = parts[0, s]
            for x in range(1, nf):
                total = total + parts[x, s]
            shares.append(total)
        return jnp.sum(jnp.concatenate(shares, axis=0), axis=1, keepdims=True)

    re, im = fsum[fme, 0], fsum[fme, 1]
    for d in range(nf - 1):
        re = re + frecv[d, 0]
        im = im + frecv[d, 1]
    ratio = jnp.transpose((re * re + im * im) / whole_norm(fnall))
    fsnr[...] = jnp.max(ratio.reshape(LF, rows, q), axis=0)
    bcopies = back_copies()
    for copy in bcopies:
        copy.start()
    back[me] = fsnr[...]

    for copy in coarse_copies:
        copy.wait_recv()
    acc = cacc[fme]
    for d in range(nf - 1):
        acc = acc + crecv[d].astype(F32)
    re, im = acc[:, :nc], acc[:, nc:]
    top = peak(re * re + im * im, segs)
    csnr[...] = jnp.transpose(top[:, :128] / whole_norm(cnall))[:segs]

    for copy in coarse_copies + norm_copies + fine_copies:
        copy.wait_send()
    for hop in range(nb - 1):
        for c in range(chunks):

            @pl.when(has_right & (me - hop >= 0))
            def _():
                ag_right(hop, c).wait_send()

            @pl.when(has_left & (me + hop < nb))
            def _():
                ag_left(hop, c).wait_send()

    @pl.loop(0, couples)
    def _(g):
        for d in range(1, nb):
            slot_couple(d, g).wait_send()

    for k in range(2):
        for d in range(1, nb):
            slot_last(d, k).wait_send()

    for copy in bcopies:
        copy.wait()
    pair_at = lax.broadcasted_iota(I32, (pairs, nb * rows), 0)
    place = jnp.zeros(pair_at.shape, I32)
    for p in range(pairs):
        place = jnp.where(pair_at == p, own[p] * rows + me * CAP + own_rank[p], place)
    giver = jnp.where(lax.broadcasted_iota(I32, place.shape, 1) == place, 1.0, 0.0)
    fout[...] = lax.dot_general(
        giver, back[...].reshape(nb * rows, q), (((1,), (0,)), ((), ())),
        precision=lax.Precision.HIGHEST, preferred_element_type=F32,
    )


def body(
    coarse_spectra,
    fine_spectra,
    coarse_templates,
    fine_templates,
    coarse_weight,
    fine_weight,
    triggers,
    offsets,
):
    nb = lax.axis_size("bank")
    nf = lax.axis_size("freq")
    ns = lax.axis_size("seg")
    seg_local = fine_spectra.shape[0]
    cbins = coarse_spectra.shape[2]
    fbins = fine_spectra.shape[2]
    top_count = triggers.shape[1]
    sub_width = fine_templates.shape[2]
    ctemps = coarse_templates.shape[1]
    rows = nb * CAP
    segs = nb * seg_local
    kc = min(1024, cbins // 2)
    kf = min(2048, fbins // 2)
    chunks = cbins // kc // 2
    csteps = cbins // kc
    fsteps = fbins // kf
    crow = ctemps // nf
    q = sub_width // nf
    period = 2 * fbins * nf
    fsplit = ns if q // ns % 16 == 0 else 1
    assert period & (period - 1) == 0 and csteps % 2 == 0 and fsteps % 2 == 0
    nc = segs * LC
    nfl = rows * LF
    ctable = jnp.asarray(unit_table(cbins * nf, CSTRIDE, 2 * cbins * nf))
    ftable = jnp.asarray(unit_table(fbins * nf, 1, period))

    vmem, anywhere = pl.BlockSpec(memory_space=pltpu.VMEM), pl.BlockSpec(memory_space=pl.ANY)
    dma = pltpu.SemaphoreType.DMA
    lag_buf = pltpu.VMEM((nc, kc), BF16)
    fine_buf = pltpu.VMEM((2 * nfl, kf), BF16)
    csnr, fine_rows = pl.pallas_call(
        functools.partial(kernel, (nb, nf, ns, fsplit, kc, kf, chunks, period)),
        out_shape=(
            pltpu.VMEM((segs, crow), F32),
            pltpu.VMEM((seg_local * top_count, q), F32),
        ),
        in_specs=[anywhere] * 10,
        out_specs=(vmem, vmem),
        scratch_shapes=[
            pltpu.SMEM((top_count, triggers.shape[0]), I32),
            pltpu.SMEM((top_count, triggers.shape[0]), I32),
            pltpu.VMEM(coarse_spectra.shape, BF16),
            pltpu.VMEM(fine_spectra.shape, BF16),
            pltpu.VMEM(coarse_templates.shape, BF16),
            pltpu.VMEM(fine_templates.shape, BF16),
            pltpu.VMEM((1, cbins), F32),
            pltpu.VMEM((1, fbins), F32),
            pltpu.VMEM((2, cbins), F32),
            pltpu.VMEM((2, fbins), F32),
            pltpu.VMEM((nb, 2 * seg_local, cbins), BF16),
            pltpu.VMEM((nb, 2 * CAP, fbins), BF16),
            pltpu.VMEM((nb, 2 * CAP, fbins), BF16),
            lag_buf, lag_buf, lag_buf, lag_buf, lag_buf, lag_buf,
            fine_buf, fine_buf,
            pltpu.VMEM((nf, crow, 2 * nc), F32),
            pltpu.VMEM((nf, crow // ns, 128), F32),
            pltpu.VMEM((nf, ns, crow // ns, 128), F32),
            pltpu.VMEM((2 * sub_width, 2 * nfl), F32),
            pltpu.VMEM((nf, 2, q, nfl), F32),
            pltpu.VMEM((nf, q // fsplit, 128), F32),
            pltpu.VMEM((nf, fsplit, q // fsplit, 128), F32),
            pltpu.VMEM((rows, q), F32),
            pltpu.VMEM((nb, rows, q), F32),
            pltpu.VMEM((nf, crow, 2 * nc), BF16),
            pltpu.VMEM((nf - 1, crow, 2 * nc), BF16),
            pltpu.VMEM((nf - 1, 2, q, nfl), F32),
            dma((8,)),
            dma((csteps,)),
            dma((fsteps,)),
            dma((nb - 1, chunks)),
            dma((nb - 1, chunks)),
            dma((nb - 1, chunks)),
            dma((nb - 1, chunks)),
            dma((nb - 1, fsteps // 2 + 1)),
            dma((nb - 1, fsteps // 2 + 1)),
            dma((nf - 1, 1)),
            dma((nf - 1, 1)),
            dma((nf * ns, 2)),
            dma((nf * ns, 2)),
            dma((nf - 1, 1)),
            dma((nf - 1, 1)),
            dma((nb - 1,)),
            dma((nb - 1,)),
        ],
        compiler_params=pltpu.CompilerParams(
            collective_id=0,
            has_side_effects=True,
            vmem_limit_bytes=60 * 1024 * 1024,
        ),
    )(
        triggers.T,
        offsets.T,
        coarse_spectra,
        fine_spectra,
        coarse_templates,
        fine_templates,
        coarse_weight[None, :],
        fine_weight[None, :],
        ctable,
        ftable,
    )
    return (csnr.T, fine_rows.reshape(seg_local, top_count, q))


def solution(mesh):
    return jax.shard_map(
        body,
        mesh=mesh,
        in_specs=(
            P(("groups", "seg", "bank"), None, "freq"),
            P(("groups", "seg", "bank"), None, "freq"),
            P(None, "bank", "freq"),
            P(None, "bank", None, "freq"),
            P(("groups", "freq")),
            P(("groups", "freq")),
            P(("groups", "seg"), None),
            P(("groups", "seg"), None),
        ),
        out_specs=(
            P(("bank", "freq"), ("groups", "seg")),
            P(("groups", "seg", "bank"), None, "freq"),
        ),
        check_vma=False,
    )
```

```python
import functools
import math

import jax
import jax.numpy as jnp
import numpy as np
from jax import lax
from jax.experimental import pallas as pl
from jax.experimental.pallas import tpu as pltpu
from jax.sharding import PartitionSpec as P

CAP = 2
LC = 16
LF = 16
CSTRIDE = 2047

MESH = pl.DeviceIdType.MESH
F32 = jnp.float32
BF16 = jnp.bfloat16
I32 = jnp.int32


def unit_table(count, stride, period):
    angle = 2.0 * np.pi * ((np.arange(count) * stride) % period) / period
    return np.stack([np.cos(angle), np.sin(angle)]).astype(np.float32)


def nt_dot(left, right):
    return lax.dot_general(left, right, (((1,), (1,)), ((), ())), preferred_element_type=F32)


def lag_series(real, imag, cos, sin, lags, emit):
    emit(0, real, imag)
    prev_re, prev_im = real, imag
    real, imag = real * cos - imag * sin, real * sin + imag * cos
    twice = cos + cos
    for j in range(1, lags):
        emit(j, real, imag)
        if j + 1 < lags:
            next_re = twice * real - prev_re
            next_im = twice * imag - prev_im
            prev_re, prev_im, real, imag = real, imag, next_re, next_im


def peak(energy, width):
    total = energy.shape[1]
    while total > width:
        half = total // 2
        if half % 128 == 0:
            energy = jnp.maximum(energy[:, :half], energy[:, half:])
        else:
            energy = jnp.maximum(energy, pltpu.roll(energy, energy.shape[1] - half, 1))
        total = half
    return energy


def kernel(cfg, *refs):
    nb, nf, ns, fsplit, kc, kf, chunks, period = cfg
    (
        trig_h, offs_h, coarse, fine, ctemp, ftemp, cweight, fweight, ctable, ftable,
        csnr, fout,
        trig, offs, coarse_v, fine_v, ctemp_v, ftemp_v, cw, fw, cstep, fstep,
        ag, outgoing, slots,
        cre0, cim0, cnre0, cre1, cim1, cnre1, fl0, fl1,
        cacc, cnorm, cnall, facc, fsum, fnorm, fnall, fsnr, back,
        crecv, frecv,
        in_sem, ct_sem, ft_sem,
        agr_send, agr_recv, agl_send, agl_recv, sl_send, sl_recv,
        cx_send, cx_recv, nx_send, nx_recv, fx_send, fx_recv, bk_send, bk_recv,
    ) = refs
    me = lax.axis_index("bank")
    fme = lax.axis_index("freq")
    sme = lax.axis_index("seg")
    seg_dev = coarse_v.shape[0]
    segs = nb * seg_dev
    rows = nb * CAP
    cbins = coarse_v.shape[2]
    fbins = fine_v.shape[2]
    csteps = cbins // kc
    fsteps = fbins // kf
    ctemps = ctemp_v.shape[1]
    sub_width = ftemp_v.shape[2]
    crow = ctemps // nf
    q = sub_width // nf
    fshare = q // fsplit
    nc = segs * LC
    nfl = rows * LF
    top_count = trig.shape[0]
    pairs = seg_dev * top_count
    cw_ag = cbins // chunks

    def win(i, width):
        return pl.ds(pl.multiple_of(i * width, width), width)

    small = [
        pltpu.make_async_copy(coarse, coarse_v, in_sem.at[0]),
        pltpu.make_async_copy(trig_h, trig, in_sem.at[6]),
        pltpu.make_async_copy(offs_h, offs, in_sem.at[7]),
        pltpu.make_async_copy(fine, fine_v, in_sem.at[1]),
        pltpu.make_async_copy(cweight, cw, in_sem.at[2]),
        pltpu.make_async_copy(fweight, fw, in_sem.at[3]),
        pltpu.make_async_copy(ctable.at[:, win(fme, cbins)], cstep, in_sem.at[4]),
        pltpu.make_async_copy(ftable.at[:, win(fme, fbins)], fstep, in_sem.at[5]),
    ]

    def ct_copy(i):
        return pltpu.make_async_copy(
            ctemp.at[:, :, win(i, kc)], ctemp_v.at[:, :, win(i, kc)], ct_sem.at[i]
        )

    def ft_copy(i):
        return pltpu.make_async_copy(
            ftemp.at[:, :, :, win(i, kf)], ftemp_v.at[:, :, :, win(i, kf)], ft_sem.at[i]
        )

    def ag_right(hop, chunk, block=None):
        block = me - hop if block is None else block
        view = ag.at[block, :, win(chunk, cw_ag)]
        return pltpu.make_async_remote_copy(
            src_ref=view, dst_ref=view,
            send_sem=agr_send.at[hop, chunk], recv_sem=agr_recv.at[hop, chunk],
            device_id={"bank": me + 1}, device_id_type=MESH,
        )

    def ag_left(hop, chunk, block=None):
        block = me + hop if block is None else block
        view = ag.at[block, :, win(chunk, cw_ag)]
        return pltpu.make_async_remote_copy(
            src_ref=view, dst_ref=view,
            send_sem=agl_send.at[hop, chunk], recv_sem=agl_recv.at[hop, chunk],
            device_id={"bank": me - 1}, device_id_type=MESH,
        )

    has_right = me + 1 < nb
    has_left = me >= 1

    couples = fsteps // 2 - 1

    def slot_copy(d, place, start, width):
        peer = lax.rem(me + d, nb)
        window = pl.ds(pl.multiple_of(start, kf), width)
        return pltpu.make_async_remote_copy(
            src_ref=outgoing.at[peer, :, window],
            dst_ref=slots.at[me, :, window],
            send_sem=sl_send.at[d - 1, place], recv_sem=sl_recv.at[d - 1, place],
            device_id={"bank": peer}, device_id_type=MESH,
        )

    def slot_couple(d, g):
        return slot_copy(d, g, g * 2 * kf, 2 * kf)

    def slot_last(d, k):
        return slot_copy(d, couples + k, (2 * couples + k) * kf, kf)

    def freq_copies(pairs_of, send, recv):
        copies = []
        for d in range(1, nf):
            peer = lax.rem(fme + d, nf)
            for k, (source, target) in enumerate(pairs_of):
                copies.append(
                    pltpu.make_async_remote_copy(
                        src_ref=source.at[peer], dst_ref=target.at[d - 1],
                        send_sem=send.at[d - 1, k], recv_sem=recv.at[d - 1, k],
                        device_id={"freq": peer}, device_id_type=MESH,
                    )
                )
        return copies

    def back_copies():
        return [
            pltpu.make_async_remote_copy(
                src_ref=fsnr, dst_ref=back.at[me],
                send_sem=bk_send.at[d - 1], recv_sem=bk_recv.at[d - 1],
                device_id={"bank": lax.rem(me + d, nb)}, device_id_type=MESH,
            )
            for d in range(1, nb)
        ]

    def by_part(block):
        block = block.astype(F32)
        return jnp.concatenate([block[:, 0, :], block[:, 1, :]], axis=0).astype(BF16)

    barrier = pltpu.get_barrier_semaphore()
    for d in range(1, nb):
        pl.semaphore_signal(
            barrier, inc=1, device_id={"bank": lax.rem(me + d, nb)}, device_id_type=MESH
        )
    for d in range(1, nf * ns):
        x, s = lax.rem(fme + d // ns, nf), lax.rem(sme + d % ns, ns)
        pl.semaphore_signal(
            barrier, inc=1, device_id={"freq": x, "seg": s}, device_id_type=MESH
        )
    for copy in small:
        copy.start()
    for i in range(csteps):
        ct_copy(i).start(priority=1)
        for k in range(i * fsteps // csteps, (i + 1) * fsteps // csteps):
            ft_copy(k).start(priority=1)
    small[0].wait()
    for c in range(chunks):
        ag[me, :, c * cw_ag : (c + 1) * cw_ag] = by_part(
            coarse_v[:, :, c * cw_ag : (c + 1) * cw_ag]
        )
    pl.semaphore_wait(barrier, nb - 1 + nf * ns - 1)
    for c in range(chunks):

        @pl.when(has_right)
        def _():
            ag_right(0, c).start()

        @pl.when(has_left)
        def _():
            ag_left(0, c).start()

    small[1].wait()
    own = [trig[p % top_count, me * seg_dev + p // top_count] for p in range(pairs)]

    def ranks_of(named):
        ranks = []
        for p in range(pairs):
            rank = jnp.int32(0)
            for before in range(p):
                rank = rank + (named[before] == named[p]).astype(I32)
            ranks.append(rank)
        return ranks

    own_rank = ranks_of(own)
    depth = 2 * CAP
    chooser_at = lax.broadcasted_iota(I32, (nb * depth, 2 * seg_dev), 0)
    chosen_col = jnp.zeros_like(chooser_at)
    for b in range(nb):
        for c in range(CAP):
            seg = jnp.int32(0)
            for p in range(pairs):
                hit = (own[p] == b) & (own_rank[p] == c)
                seg = jnp.where(hit, jnp.int32(p // top_count), seg)
            for part in range(2):
                chosen_col = jnp.where(
                    chooser_at == b * depth + part * CAP + c, seg + part * seg_dev, chosen_col
                )
    choice = jnp.where(
        lax.broadcasted_iota(I32, chooser_at.shape, 1) == chosen_col, 1.0, 0.0
    ).astype(BF16)

    small[3].wait()
    group = 2

    @pl.loop(0, fsteps // group)
    def _(i):
        for g in range(group):
            window = win(i * group + g, kf)
            chosen = jnp.dot(
                choice, by_part(fine_v[:, :, window]), preferred_element_type=F32
            ).astype(BF16)
            for b in range(nb):
                outgoing[b, :, window] = chosen[b * depth : (b + 1) * depth]

    slots[me] = outgoing[me]
    for copy in small[2:3] + small[4:]:
        copy.wait()

    cnorm[...] = jnp.zeros_like(cnorm)
    fnorm[...] = jnp.zeros_like(fnorm)
    cacc[...] = jnp.zeros_like(cacc)
    facc[...] = jnp.zeros_like(facc)

    cshare = crow // ns

    def norm_rows(acc, k, place, temps, start, bins, width, weight):
        part = None
        rows_at = pl.ds(pl.multiple_of(start, 16), 16)
        for c in range(0, width, 128):
            lanes = pl.ds(pl.multiple_of(bins + c, 128), 128)
            hr, hi = temps(rows_at, lanes)
            hr, hi = hr.astype(F32), hi.astype(F32)
            term = (hr * hr + hi * hi) * weight[:, c : c + 128]
            part = term if part is None else part + term
        acc[k, place : place + 16, :] += part

    def coarse_norm(i):
        ct_copy(i).wait()
        weight = cw[:, win(i, kc)]
        for k in range(nf):
            for r in range(0, cshare, 16):
                norm_rows(
                    cnorm, k, r,
                    lambda rows_at, lanes: (ctemp_v[0, rows_at, lanes], ctemp_v[1, rows_at, lanes]),
                    k * crow + sme * cshare + r, i * kc, kc, weight,
                )

    def fine_norm(i):
        ft_copy(i).wait()
        weight = fw[:, win(i, kf)]
        for k in range(nf):
            for r in range(0, fshare, 16):
                norm_rows(
                    fnorm, k, r,
                    lambda rows_at, lanes: (
                        ftemp_v[0, 0, rows_at, lanes], ftemp_v[1, 0, rows_at, lanes],
                    ),
                    k * q + (sme * fshare if fsplit > 1 else 0) + r, i * kf, kf, weight,
                )

    def send_slots(rightward, dists, low, high):
        def send(dist, copy):
            there = me + dist < nb if rightward else me >= dist

            @pl.when(there)
            def _():
                copy(dist if rightward else nb - dist).start()

        @pl.loop(low, min(high, couples))
        def _(g):
            for dist in dists:
                send(dist, lambda d: slot_couple(d, g))

        if high > couples:
            for k in range(2):
                for dist in dists:
                    send(dist, lambda d: slot_last(d, k))

    def slots_off(rightward, end):
        if end:
            send_slots(rightward, [1], 0, couples + 1)
            send_slots(rightward, range(2, nb), 0, couples + 1)
        else:
            send_slots(rightward, range(1, nb), 1, couples + 1)

    @pl.when(me > 0)
    def _():
        send_slots(True, range(1, nb), 0, 1)

    @pl.when(me < nb - 1)
    def _():
        send_slots(False, range(1, nb), 0, 1)

    def gathered_chunk(hop, c):
        @pl.when(me - 1 - hop >= 0)
        def _():
            ag_right(hop, c, me - 1 - hop).wait_recv()

            @pl.when(has_right)
            def _():
                ag_right(hop + 1, c).start()

        @pl.when(me + 1 + hop < nb)
        def _():
            ag_left(hop, c, me + 1 + hop).wait_recv()

            @pl.when(has_left)
            def _():
                ag_left(hop + 1, c).start()

        if c == chunks - 1:

            @pl.when(me == hop + 1)
            def _():
                slots_off(True, False)

            @pl.when(nb - 1 - me == hop + 1)
            def _():
                slots_off(False, False)

    @pl.when(me == 0)
    def _():
        slots_off(True, True)

    @pl.when(me == nb - 1)
    def _():
        slots_off(False, True)

    events = [(hop, c) for hop in range(nb - 2) for c in range(chunks)]
    per = fsteps // csteps
    first = 3 * csteps // 8

    @pl.loop(0, csteps)
    def _(i):
        coarse_norm(i)
        for at in range(first, csteps):

            @pl.when(i == at)
            def _():
                gathered_chunk(*events[at - first])

        for k in range(per):
            fine_norm(i * per + k)

    cnall[fme, sme] = cnorm[fme]
    fnall[fme, sme if fsplit > 1 else 0] = fnorm[fme]
    norm_copies = []
    for dx in range(nf):
        for ds in range(ns):
            if dx + ds == 0:
                continue
            x, s = lax.rem(fme + dx, nf), lax.rem(sme + ds, ns)
            kinds = [(cnorm, cnall, sme)]
            if fsplit > 1 or ds == 0:
                kinds.append((fnorm, fnall, sme if fsplit > 1 else 0))
            for kind, (source, target, at) in enumerate(kinds):
                norm_copies.append(
                    pltpu.make_async_remote_copy(
                        src_ref=source.at[x], dst_ref=target.at[fme, at],
                        send_sem=nx_send.at[dx * ns + ds, kind],
                        recv_sem=nx_recv.at[dx * ns + ds, kind],
                        device_id={"freq": x, "seg": s}, device_id_type=MESH,
                    )
                )
    for copy in norm_copies:
        copy.start()
    for event in events[csteps - first :]:
        gathered_chunk(*event)

    cbuf = ((cre0, cim0, cnre0), (cre1, cim1, cnre1))

    def coarse_lags(i, buf):
        re_ref, im_ref, nre_ref = buf
        sub = 256
        for c in range(0, kc, sub):
            window = pl.ds(pl.multiple_of(i * kc + c, sub), sub)
            blocks = [ag[b, :, window].astype(F32) for b in range(nb)]
            w = cw[:, window]
            real = jnp.concatenate([x[:seg_dev] for x in blocks], axis=0) * w
            imag = jnp.concatenate([x[seg_dev:] for x in blocks], axis=0) * w

            def emit(j, re, im):
                re = re.astype(BF16)
                re_ref[j * segs : (j + 1) * segs, c : c + sub] = re
                nre_ref[j * segs : (j + 1) * segs, c : c + sub] = -re
                im_ref[j * segs : (j + 1) * segs, c : c + sub] = im.astype(BF16)

            lag_series(real, imag, cstep[0:1, window], cstep[1:2, window], LC, emit)

    def coarse_products(i, buf):
        re_ref, im_ref, nre_ref = buf
        window = win(i, kc)
        left = jnp.concatenate([ctemp_v[0, :, window], ctemp_v[1, :, window]], axis=1)
        re, im, nre = re_ref[...], im_ref[...], nre_ref[...]
        right = jnp.concatenate(
            [jnp.concatenate([re, im], axis=1), jnp.concatenate([im, nre], axis=1)], axis=0
        )
        out = nt_dot(left, right)
        for k in range(nf):
            cacc[k] += out[k * crow : (k + 1) * crow]

    def last_hop(c):
        @pl.when(me == nb - 1)
        def _():
            ag_right(nb - 2, c, 0).wait_recv()

        @pl.when(me == 0)
        def _():
            ag_left(nb - 2, c, nb - 1).wait_recv()

    last_hop(0)
    coarse_lags(0, cbuf[0])

    @pl.loop(0, csteps // 2)
    def _(i):
        @pl.when(i + 1 < chunks)
        def _():
            last_hop(i + 1)

        coarse_lags(2 * i + 1, cbuf[1])
        coarse_products(2 * i, cbuf[0])
        coarse_lags(jnp.minimum(2 * i + 2, csteps - 1), cbuf[0])
        coarse_products(2 * i + 1, cbuf[1])

    coarse_copies = freq_copies(((cacc, crecv),), cx_send, cx_recv)
    for copy in coarse_copies:
        copy.start()

    row_at = lax.broadcasted_iota(I32, (rows, 128), 0)
    shift = jnp.zeros((rows, 128), I32)
    for b in range(nb):
        block = [trig[p % top_count, b * seg_dev + p // top_count] for p in range(pairs)]
        taken = jnp.int32(0)
        for p in range(pairs):
            hit = block[p] == me
            offset = offs[p % top_count, b * seg_dev + p // top_count]
            shift = jnp.where(
                row_at == jnp.where(hit, b * CAP + taken, -1), offset, shift
            )
            taken = taken + hit.astype(I32)
    lane = lax.broadcasted_iota(I32, (rows, 128), 1)
    tiles = fbins // 128
    lane_angle = ((shift * lane) & (period - 1)).astype(F32) * (2.0 * math.pi / period)
    lane_cos, lane_sin = jnp.cos(lane_angle), jnp.sin(lane_angle)
    coarse_period = period // 128
    tile_at = lax.broadcasted_iota(I32, (rows, tiles), 1) + fme * tiles
    wide = jnp.concatenate([shift] * (tiles // 128), axis=1)
    tile_angle = ((wide * tile_at) & (coarse_period - 1)).astype(F32) * (
        2.0 * math.pi / coarse_period
    )
    tile_cos, tile_sin = jnp.cos(tile_angle), jnp.sin(tile_angle)

    def fine_lags(i, buf):
        per = kf // 128
        turn = lax.rem(tiles - i * per, tiles)
        here_cos = pltpu.roll(tile_cos, turn, 1)
        here_sin = pltpu.roll(tile_sin, turn, 1)
        sub = 512
        for c in range(0, kf, sub):
            window = pl.ds(pl.multiple_of(i * kf + c, sub), sub)
            blocks = [slots[b, :, window].astype(F32) for b in range(nb)]
            w = fw[:, window]
            real = jnp.concatenate([x[:CAP] for x in blocks], axis=0) * w
            imag = jnp.concatenate([x[CAP:] for x in blocks], axis=0) * w
            turn_re, turn_im = [], []
            for t in range(c // 128, (c + sub) // 128):
                a_cos = here_cos[:, t : t + 1]
                a_sin = here_sin[:, t : t + 1]
                turn_re.append(a_cos * lane_cos - a_sin * lane_sin)
                turn_im.append(a_cos * lane_sin + a_sin * lane_cos)
            sr = jnp.concatenate(turn_re, axis=1)
            si = jnp.concatenate(turn_im, axis=1)
            real, imag = real * sr - imag * si, real * si + imag * sr
            held = []

            def emit(j, re, im):
                held.append((re, im))
                if len(held) == 2:
                    low, high = (j - 1) * rows, (j + 1) * rows
                    buf[low:high, c : c + sub] = jnp.concatenate(
                        [held[0][0], held[1][0]], axis=0
                    ).astype(BF16)
                    buf[nfl + low : nfl + high, c : c + sub] = jnp.concatenate(
                        [held[0][1], held[1][1]], axis=0
                    ).astype(BF16)
                    held.clear()

            lag_series(real, imag, fstep[0:1, window], fstep[1:2, window], LF, emit)

    def fine_products(i, buf):
        window = win(i, kf)
        left = jnp.concatenate([ftemp_v[0, 0, :, window], ftemp_v[1, 0, :, window]], axis=0)
        facc[...] += nt_dot(left, buf[...])

    def slots_here(copy, at):
        for d in range(1, nb):
            copy(d, at).wait_recv()

    slots_here(slot_couple, 0)
    fine_lags(0, fl0)

    @pl.loop(0, fsteps // 2 - 1)
    def _(i):
        @pl.when(i + 1 < couples)
        def _():
            slots_here(slot_couple, i + 1)

        @pl.when(i + 1 == couples)
        def _():
            slots_here(slot_last, 0)

        fine_lags(2 * i + 1, fl1)
        fine_products(2 * i, fl0)
        fine_lags(2 * i + 2, fl0)
        fine_products(2 * i + 1, fl1)

    slots_here(slot_last, 1)
    fine_lags(fsteps - 1, fl1)
    fine_products(fsteps - 2, fl0)
    fine_products(fsteps - 1, fl1)

    both = facc.shape[0] // 2
    re = facc[:both, :nfl] + facc[both:, nfl:]
    im = facc[:both, nfl:] - facc[both:, :nfl]
    for k in range(nf):
        fsum[k, 0] = re[k * q : (k + 1) * q]
        fsum[k, 1] = im[k * q : (k + 1) * q]
    fine_copies = freq_copies(((fsum, frecv),), fx_send, fx_recv)
    for copy in fine_copies:
        copy.start()
    for copy in norm_copies + fine_copies:
        copy.wait_recv()
    def whole_norm(parts):
        shares = []
        for s in range(parts.shape[1]):
            total = parts[0, s]
            for x in range(1, nf):
                total = total + parts[x, s]
            shares.append(total)
        return jnp.sum(jnp.concatenate(shares, axis=0), axis=1, keepdims=True)

    re, im = fsum[fme, 0], fsum[fme, 1]
    for d in range(nf - 1):
        re = re + frecv[d, 0]
        im = im + frecv[d, 1]
    ratio = jnp.transpose((re * re + im * im) / whole_norm(fnall))
    fsnr[...] = jnp.max(ratio.reshape(LF, rows, q), axis=0)
    bcopies = back_copies()
    for copy in bcopies:
        copy.start()
    back[me] = fsnr[...]

    for copy in coarse_copies:
        copy.wait_recv()
    acc = cacc[fme]
    for d in range(nf - 1):
        acc = acc + crecv[d]
    re, im = acc[:, :nc], acc[:, nc:]
    top = peak(re * re + im * im, segs)
    csnr[...] = jnp.transpose(top[:, :128] / whole_norm(cnall))[:segs]

    for copy in coarse_copies + norm_copies + fine_copies:
        copy.wait_send()
    for hop in range(nb - 1):
        for c in range(chunks):

            @pl.when(has_right & (me - hop >= 0))
            def _():
                ag_right(hop, c).wait_send()

            @pl.when(has_left & (me + hop < nb))
            def _():
                ag_left(hop, c).wait_send()

    @pl.loop(0, couples)
    def _(g):
        for d in range(1, nb):
            slot_couple(d, g).wait_send()

    for k in range(2):
        for d in range(1, nb):
            slot_last(d, k).wait_send()

    for copy in bcopies:
        copy.wait()
    pair_at = lax.broadcasted_iota(I32, (pairs, nb * rows), 0)
    place = jnp.zeros(pair_at.shape, I32)
    for p in range(pairs):
        place = jnp.where(pair_at == p, own[p] * rows + me * CAP + own_rank[p], place)
    giver = jnp.where(lax.broadcasted_iota(I32, place.shape, 1) == place, 1.0, 0.0)
    fout[...] = lax.dot_general(
        giver, back[...].reshape(nb * rows, q), (((1,), (0,)), ((), ())),
        precision=lax.Precision.HIGHEST, preferred_element_type=F32,
    )


def body(
    coarse_spectra,
    fine_spectra,
    coarse_templates,
    fine_templates,
    coarse_weight,
    fine_weight,
    triggers,
    offsets,
):
    nb = lax.axis_size("bank")
    nf = lax.axis_size("freq")
    ns = lax.axis_size("seg")
    seg_local = fine_spectra.shape[0]
    cbins = coarse_spectra.shape[2]
    fbins = fine_spectra.shape[2]
    top_count = triggers.shape[1]
    sub_width = fine_templates.shape[2]
    ctemps = coarse_templates.shape[1]
    rows = nb * CAP
    segs = nb * seg_local
    kc = min(1024, cbins // 2)
    kf = min(2048, fbins // 2)
    chunks = cbins // kc // 2
    csteps = cbins // kc
    fsteps = fbins // kf
    crow = ctemps // nf
    q = sub_width // nf
    period = 2 * fbins * nf
    fsplit = ns if q // ns % 16 == 0 else 1
    assert period & (period - 1) == 0 and csteps % 2 == 0 and fsteps % 2 == 0
    nc = segs * LC
    nfl = rows * LF
    ctable = jnp.asarray(unit_table(cbins * nf, CSTRIDE, 2 * cbins * nf))
    ftable = jnp.asarray(unit_table(fbins * nf, 1, period))

    vmem, anywhere = pl.BlockSpec(memory_space=pltpu.VMEM), pl.BlockSpec(memory_space=pl.ANY)
    dma = pltpu.SemaphoreType.DMA
    lag_buf = pltpu.VMEM((nc, kc), BF16)
    fine_buf = pltpu.VMEM((2 * nfl, kf), BF16)
    csnr, fine_rows = pl.pallas_call(
        functools.partial(kernel, (nb, nf, ns, fsplit, kc, kf, chunks, period)),
        out_shape=(
            pltpu.VMEM((segs, crow), F32),
            pltpu.VMEM((seg_local * top_count, q), F32),
        ),
        in_specs=[anywhere] * 10,
        out_specs=(vmem, vmem),
        scratch_shapes=[
            pltpu.SMEM((top_count, triggers.shape[0]), I32),
            pltpu.SMEM((top_count, triggers.shape[0]), I32),
            pltpu.VMEM(coarse_spectra.shape, BF16),
            pltpu.VMEM(fine_spectra.shape, BF16),
            pltpu.VMEM(coarse_templates.shape, BF16),
            pltpu.VMEM(fine_templates.shape, BF16),
            pltpu.VMEM((1, cbins), F32),
            pltpu.VMEM((1, fbins), F32),
            pltpu.VMEM((2, cbins), F32),
            pltpu.VMEM((2, fbins), F32),
            pltpu.VMEM((nb, 2 * seg_local, cbins), BF16),
            pltpu.VMEM((nb, 2 * CAP, fbins), BF16),
            pltpu.VMEM((nb, 2 * CAP, fbins), BF16),
            lag_buf, lag_buf, lag_buf, lag_buf, lag_buf, lag_buf,
            fine_buf, fine_buf,
            pltpu.VMEM((nf, crow, 2 * nc), F32),
            pltpu.VMEM((nf, crow // ns, 128), F32),
            pltpu.VMEM((nf, ns, crow // ns, 128), F32),
            pltpu.VMEM((2 * sub_width, 2 * nfl), F32),
            pltpu.VMEM((nf, 2, q, nfl), F32),
            pltpu.VMEM((nf, q // fsplit, 128), F32),
            pltpu.VMEM((nf, fsplit, q // fsplit, 128), F32),
            pltpu.VMEM((rows, q), F32),
            pltpu.VMEM((nb, rows, q), F32),
            pltpu.VMEM((nf - 1, crow, 2 * nc), F32),
            pltpu.VMEM((nf - 1, 2, q, nfl), F32),
            dma((8,)),
            dma((csteps,)),
            dma((fsteps,)),
            dma((nb - 1, chunks)),
            dma((nb - 1, chunks)),
            dma((nb - 1, chunks)),
            dma((nb - 1, chunks)),
            dma((nb - 1, fsteps // 2 + 1)),
            dma((nb - 1, fsteps // 2 + 1)),
            dma((nf - 1, 1)),
            dma((nf - 1, 1)),
            dma((nf * ns, 2)),
            dma((nf * ns, 2)),
            dma((nf - 1, 1)),
            dma((nf - 1, 1)),
            dma((nb - 1,)),
            dma((nb - 1,)),
        ],
        compiler_params=pltpu.CompilerParams(
            collective_id=0,
            has_side_effects=True,
            vmem_limit_bytes=60 * 1024 * 1024,
        ),
    )(
        triggers.T,
        offsets.T,
        coarse_spectra,
        fine_spectra,
        coarse_templates,
        fine_templates,
        coarse_weight[None, :],
        fine_weight[None, :],
        ctable,
        ftable,
    )
    def settle(c_in, f_in, c_out, f_out, sem):
        copies = [
            pltpu.make_async_copy(c_in, c_out, sem.at[0]),
            pltpu.make_async_copy(f_in, f_out, sem.at[1]),
        ]
        for copy in copies:
            copy.start()
        for copy in copies:
            copy.wait()

    csnr, fine_rows = pl.pallas_call(
        settle,
        out_shape=(
            jax.ShapeDtypeStruct(csnr.shape, F32), jax.ShapeDtypeStruct(fine_rows.shape, F32)
        ),
        in_specs=[vmem, vmem],
        out_specs=(anywhere, anywhere),
        scratch_shapes=[dma((2,))],
    )(
        pltpu.with_memory_space_constraint(csnr, pltpu.VMEM),
        pltpu.with_memory_space_constraint(fine_rows, pltpu.VMEM),
    )
    return (csnr.T, fine_rows.reshape(seg_local, top_count, q))


def solution(mesh):
    return jax.shard_map(
        body,
        mesh=mesh,
        in_specs=(
            P(("groups", "seg", "bank"), None, "freq"),
            P(("groups", "seg", "bank"), None, "freq"),
            P(None, "bank", "freq"),
            P(None, "bank", None, "freq"),
            P(("groups", "freq")),
            P(("groups", "freq")),
            P(("groups", "seg"), None),
            P(("groups", "seg"), None),
        ),
        out_specs=(
            P(("bank", "freq"), ("groups", "seg")),
            P(("groups", "seg", "bank"), None, "freq"),
        ),
        check_vma=False,
    )
```

```python
import functools
import math

import jax
import jax.numpy as jnp
import numpy as np
from jax import lax
from jax.experimental import pallas as pl
from jax.experimental.pallas import tpu as pltpu
from jax.sharding import PartitionSpec as P

CAP = 2
LC = 16
LF = 16
CSTRIDE = 2047

MESH = pl.DeviceIdType.MESH
F32 = jnp.float32
BF16 = jnp.bfloat16
I32 = jnp.int32


def unit_table(count, stride, period):
    angle = 2.0 * np.pi * ((np.arange(count) * stride) % period) / period
    return np.stack([np.cos(angle), np.sin(angle)]).astype(np.float32)


def nt_dot(left, right):
    return lax.dot_general(left, right, (((1,), (1,)), ((), ())), preferred_element_type=F32)


def lag_series(real, imag, cos, sin, lags, emit):
    emit(0, real, imag)
    prev_re, prev_im = real, imag
    real, imag = real * cos - imag * sin, real * sin + imag * cos
    twice = cos + cos
    for j in range(1, lags):
        emit(j, real, imag)
        if j + 1 < lags:
            next_re = twice * real - prev_re
            next_im = twice * imag - prev_im
            prev_re, prev_im, real, imag = real, imag, next_re, next_im


def peak(energy, width):
    total = energy.shape[1]
    while total > width:
        half = total // 2
        if half % 128 == 0:
            energy = jnp.maximum(energy[:, :half], energy[:, half:])
        else:
            energy = jnp.maximum(energy, pltpu.roll(energy, energy.shape[1] - half, 1))
        total = half
    return energy


def kernel(cfg, *refs):
    nb, nf, ns, fsplit, kc, kf, chunks, period = cfg
    (
        trig_h, offs_h, coarse, fine, ctemp, ftemp, cweight, fweight, ctable, ftable,
        csnr, fout,
        trig, offs, coarse_v, fine_v, ctemp_v, ftemp_v, cw, fw, cstep, fstep,
        ag, outgoing, slots,
        cre0, cim0, cnre0, cre1, cim1, cnre1, fl0, fl1,
        cacc, cnorm, cnall, facc, fsum, fnorm, fnall, fsnr, back,
        crecv, frecv,
        in_sem, ct_sem, ft_sem,
        agr_send, agr_recv, agl_send, agl_recv, sl_send, sl_recv,
        cx_send, cx_recv, nx_send, nx_recv, fx_send, fx_recv, bk_send, bk_recv,
    ) = refs
    me = lax.axis_index("bank")
    fme = lax.axis_index("freq")
    sme = lax.axis_index("seg")
    seg_dev = coarse_v.shape[0]
    segs = nb * seg_dev
    rows = nb * CAP
    cbins = coarse_v.shape[2]
    fbins = fine_v.shape[2]
    csteps = cbins // kc
    fsteps = fbins // kf
    ctemps = ctemp_v.shape[1]
    sub_width = ftemp_v.shape[2]
    crow = ctemps // nf
    q = sub_width // nf
    fshare = q // fsplit
    nc = segs * LC
    nfl = rows * LF
    top_count = trig.shape[0]
    pairs = seg_dev * top_count
    cw_ag = cbins // chunks

    def win(i, width):
        return pl.ds(pl.multiple_of(i * width, width), width)

    small = [
        pltpu.make_async_copy(coarse, coarse_v, in_sem.at[0]),
        pltpu.make_async_copy(trig_h, trig, in_sem.at[6]),
        pltpu.make_async_copy(offs_h, offs, in_sem.at[7]),
        pltpu.make_async_copy(fine, fine_v, in_sem.at[1]),
        pltpu.make_async_copy(cweight, cw, in_sem.at[2]),
        pltpu.make_async_copy(fweight, fw, in_sem.at[3]),
        pltpu.make_async_copy(ctable.at[:, win(fme, cbins)], cstep, in_sem.at[4]),
        pltpu.make_async_copy(ftable.at[:, win(fme, fbins)], fstep, in_sem.at[5]),
    ]

    def ct_copy(i):
        return pltpu.make_async_copy(
            ctemp.at[:, :, win(i, kc)], ctemp_v.at[:, :, win(i, kc)], ct_sem.at[i]
        )

    def ft_copy(i):
        return pltpu.make_async_copy(
            ftemp.at[:, :, :, win(i, kf)], ftemp_v.at[:, :, :, win(i, kf)], ft_sem.at[i]
        )

    def ag_right(hop, chunk, block=None):
        block = me - hop if block is None else block
        view = ag.at[block, :, win(chunk, cw_ag)]
        return pltpu.make_async_remote_copy(
            src_ref=view, dst_ref=view,
            send_sem=agr_send.at[hop, chunk], recv_sem=agr_recv.at[hop, chunk],
            device_id={"bank": me + 1}, device_id_type=MESH,
        )

    def ag_left(hop, chunk, block=None):
        block = me + hop if block is None else block
        view = ag.at[block, :, win(chunk, cw_ag)]
        return pltpu.make_async_remote_copy(
            src_ref=view, dst_ref=view,
            send_sem=agl_send.at[hop, chunk], recv_sem=agl_recv.at[hop, chunk],
            device_id={"bank": me - 1}, device_id_type=MESH,
        )

    has_right = me + 1 < nb
    has_left = me >= 1

    couples = fsteps // 2 - 1

    def slot_copy(d, place, start, width):
        peer = lax.rem(me + d, nb)
        window = pl.ds(pl.multiple_of(start, kf), width)
        return pltpu.make_async_remote_copy(
            src_ref=outgoing.at[peer, :, window],
            dst_ref=slots.at[me, :, window],
            send_sem=sl_send.at[d - 1, place], recv_sem=sl_recv.at[d - 1, place],
            device_id={"bank": peer}, device_id_type=MESH,
        )

    def slot_couple(d, g):
        return slot_copy(d, g, g * 2 * kf, 2 * kf)

    def slot_last(d, k):
        return slot_copy(d, couples + k, (2 * couples + k) * kf, kf)

    def freq_copies(pairs_of, send, recv):
        copies = []
        for d in range(1, nf):
            peer = lax.rem(fme + d, nf)
            for k, (source, target) in enumerate(pairs_of):
                copies.append(
                    pltpu.make_async_remote_copy(
                        src_ref=source.at[peer], dst_ref=target.at[d - 1],
                        send_sem=send.at[d - 1, k], recv_sem=recv.at[d - 1, k],
                        device_id={"freq": peer}, device_id_type=MESH,
                    )
                )
        return copies

    def back_copies():
        return [
            pltpu.make_async_remote_copy(
                src_ref=fsnr, dst_ref=back.at[me],
                send_sem=bk_send.at[d - 1], recv_sem=bk_recv.at[d - 1],
                device_id={"bank": lax.rem(me + d, nb)}, device_id_type=MESH,
            )
            for d in range(1, nb)
        ]

    def by_part(block):
        block = block.astype(F32)
        return jnp.concatenate([block[:, 0, :], block[:, 1, :]], axis=0).astype(BF16)

    barrier = pltpu.get_barrier_semaphore()
    for d in range(1, nb):
        pl.semaphore_signal(
            barrier, inc=1, device_id={"bank": lax.rem(me + d, nb)}, device_id_type=MESH
        )
    for d in range(1, nf * ns):
        x, s = lax.rem(fme + d // ns, nf), lax.rem(sme + d % ns, ns)
        pl.semaphore_signal(
            barrier, inc=1, device_id={"freq": x, "seg": s}, device_id_type=MESH
        )
    for copy in small:
        copy.start()
    for i in range(csteps):
        ct_copy(i).start(priority=1)
        for k in range(i * fsteps // csteps, (i + 1) * fsteps // csteps):
            ft_copy(k).start(priority=1)
    small[0].wait()
    for c in range(chunks):
        ag[me, :, c * cw_ag : (c + 1) * cw_ag] = by_part(
            coarse_v[:, :, c * cw_ag : (c + 1) * cw_ag]
        )
    pl.semaphore_wait(barrier, nb - 1 + nf * ns - 1)
    for c in range(chunks):

        @pl.when(has_right)
        def _():
            ag_right(0, c).start()

        @pl.when(has_left)
        def _():
            ag_left(0, c).start()

    small[1].wait()
    own = [trig[p % top_count, me * seg_dev + p // top_count] for p in range(pairs)]

    def ranks_of(named):
        ranks = []
        for p in range(pairs):
            rank = jnp.int32(0)
            for before in range(p):
                rank = rank + (named[before] == named[p]).astype(I32)
            ranks.append(rank)
        return ranks

    own_rank = ranks_of(own)
    depth = 2 * CAP
    chooser_at = lax.broadcasted_iota(I32, (nb * depth, 2 * seg_dev), 0)
    chosen_col = jnp.zeros_like(chooser_at)
    for b in range(nb):
        for c in range(CAP):
            seg = jnp.int32(0)
            for p in range(pairs):
                hit = (own[p] == b) & (own_rank[p] == c)
                seg = jnp.where(hit, jnp.int32(p // top_count), seg)
            for part in range(2):
                chosen_col = jnp.where(
                    chooser_at == b * depth + part * CAP + c, seg + part * seg_dev, chosen_col
                )
    choice = jnp.where(
        lax.broadcasted_iota(I32, chooser_at.shape, 1) == chosen_col, 1.0, 0.0
    ).astype(BF16)

    small[3].wait()
    group = 2

    @pl.loop(0, fsteps // group)
    def _(i):
        for g in range(group):
            window = win(i * group + g, kf)
            chosen = jnp.dot(
                choice, by_part(fine_v[:, :, window]), preferred_element_type=F32
            ).astype(BF16)
            for b in range(nb):
                outgoing[b, :, window] = chosen[b * depth : (b + 1) * depth]

    slots[me] = outgoing[me]
    for copy in small[2:3] + small[4:]:
        copy.wait()

    cnorm[...] = jnp.zeros_like(cnorm)
    fnorm[...] = jnp.zeros_like(fnorm)
    cacc[...] = jnp.zeros_like(cacc)
    facc[...] = jnp.zeros_like(facc)

    cshare = crow // ns

    def norm_rows(acc, k, place, temps, start, bins, width, weight):
        part = None
        rows_at = pl.ds(pl.multiple_of(start, 16), 16)
        for c in range(0, width, 128):
            lanes = pl.ds(pl.multiple_of(bins + c, 128), 128)
            hr, hi = temps(rows_at, lanes)
            hr, hi = hr.astype(F32), hi.astype(F32)
            term = (hr * hr + hi * hi) * weight[:, c : c + 128]
            part = term if part is None else part + term
        acc[k, place : place + 16, :] += part

    def coarse_norm(i):
        ct_copy(i).wait()
        weight = cw[:, win(i, kc)]
        for k in range(nf):
            for r in range(0, cshare, 16):
                norm_rows(
                    cnorm, k, r,
                    lambda rows_at, lanes: (ctemp_v[0, rows_at, lanes], ctemp_v[1, rows_at, lanes]),
                    k * crow + sme * cshare + r, i * kc, kc, weight,
                )

    def fine_norm(i):
        ft_copy(i).wait()
        weight = fw[:, win(i, kf)]
        for k in range(nf):
            for r in range(0, fshare, 16):
                norm_rows(
                    fnorm, k, r,
                    lambda rows_at, lanes: (
                        ftemp_v[0, 0, rows_at, lanes], ftemp_v[1, 0, rows_at, lanes],
                    ),
                    k * q + (sme * fshare if fsplit > 1 else 0) + r, i * kf, kf, weight,
                )

    def send_slots(rightward, dists, low, high):
        def send(dist, copy):
            there = me + dist < nb if rightward else me >= dist

            @pl.when(there)
            def _():
                copy(dist if rightward else nb - dist).start()

        @pl.loop(low, min(high, couples))
        def _(g):
            for dist in dists:
                send(dist, lambda d: slot_couple(d, g))

        if high > couples:
            for k in range(2):
                for dist in dists:
                    send(dist, lambda d: slot_last(d, k))

    def slots_off(rightward, end):
        if end:
            send_slots(rightward, [1], 0, couples + 1)
            send_slots(rightward, range(nb - 1, 1, -1), 0, couples + 1)
        else:
            send_slots(rightward, range(nb - 1, 0, -1), 1, couples + 1)

    @pl.when(me > 0)
    def _():
        send_slots(True, range(1, nb), 0, 1)

    @pl.when(me < nb - 1)
    def _():
        send_slots(False, range(1, nb), 0, 1)

    def gathered_chunk(hop, c):
        @pl.when(me - 1 - hop >= 0)
        def _():
            ag_right(hop, c, me - 1 - hop).wait_recv()

            @pl.when(has_right)
            def _():
                ag_right(hop + 1, c).start()

        @pl.when(me + 1 + hop < nb)
        def _():
            ag_left(hop, c, me + 1 + hop).wait_recv()

            @pl.when(has_left)
            def _():
                ag_left(hop + 1, c).start()

        if c == chunks - 1:

            @pl.when(me == hop + 1)
            def _():
                slots_off(True, False)

            @pl.when(nb - 1 - me == hop + 1)
            def _():
                slots_off(False, False)

    @pl.when(me == 0)
    def _():
        slots_off(True, True)

    @pl.when(me == nb - 1)
    def _():
        slots_off(False, True)

    events = [(hop, c) for hop in range(nb - 2) for c in range(chunks)]
    per = fsteps // csteps
    first = 3 * csteps // 8

    @pl.loop(0, csteps)
    def _(i):
        coarse_norm(i)
        for at in range(first, csteps):

            @pl.when(i == at)
            def _():
                gathered_chunk(*events[at - first])

        for k in range(per):
            fine_norm(i * per + k)

    cnall[fme, sme] = cnorm[fme]
    fnall[fme, sme if fsplit > 1 else 0] = fnorm[fme]
    norm_copies = []
    for dx in range(nf):
        for ds in range(ns):
            if dx + ds == 0:
                continue
            x, s = lax.rem(fme + dx, nf), lax.rem(sme + ds, ns)
            kinds = [(cnorm, cnall, sme)]
            if fsplit > 1 or ds == 0:
                kinds.append((fnorm, fnall, sme if fsplit > 1 else 0))
            for kind, (source, target, at) in enumerate(kinds):
                norm_copies.append(
                    pltpu.make_async_remote_copy(
                        src_ref=source.at[x], dst_ref=target.at[fme, at],
                        send_sem=nx_send.at[dx * ns + ds, kind],
                        recv_sem=nx_recv.at[dx * ns + ds, kind],
                        device_id={"freq": x, "seg": s}, device_id_type=MESH,
                    )
                )
    for copy in norm_copies:
        copy.start()
    for event in events[csteps - first :]:
        gathered_chunk(*event)

    cbuf = ((cre0, cim0, cnre0), (cre1, cim1, cnre1))

    def coarse_lags(i, buf):
        re_ref, im_ref, nre_ref = buf
        sub = 256
        for c in range(0, kc, sub):
            window = pl.ds(pl.multiple_of(i * kc + c, sub), sub)
            blocks = [ag[b, :, window].astype(F32) for b in range(nb)]
            w = cw[:, window]
            real = jnp.concatenate([x[:seg_dev] for x in blocks], axis=0) * w
            imag = jnp.concatenate([x[seg_dev:] for x in blocks], axis=0) * w

            def emit(j, re, im):
                re = re.astype(BF16)
                re_ref[j * segs : (j + 1) * segs, c : c + sub] = re
                nre_ref[j * segs : (j + 1) * segs, c : c + sub] = -re
                im_ref[j * segs : (j + 1) * segs, c : c + sub] = im.astype(BF16)

            lag_series(real, imag, cstep[0:1, window], cstep[1:2, window], LC, emit)

    def coarse_products(i, buf):
        re_ref, im_ref, nre_ref = buf
        window = win(i, kc)
        left = jnp.concatenate([ctemp_v[0, :, window], ctemp_v[1, :, window]], axis=1)
        re, im, nre = re_ref[...], im_ref[...], nre_ref[...]
        right = jnp.concatenate(
            [jnp.concatenate([re, im], axis=1), jnp.concatenate([im, nre], axis=1)], axis=0
        )
        out = nt_dot(left, right)
        for k in range(nf):
            cacc[k] += out[k * crow : (k + 1) * crow]

    def last_hop(c):
        @pl.when(me == nb - 1)
        def _():
            ag_right(nb - 2, c, 0).wait_recv()

        @pl.when(me == 0)
        def _():
            ag_left(nb - 2, c, nb - 1).wait_recv()

    last_hop(0)
    coarse_lags(0, cbuf[0])

    @pl.loop(0, csteps // 2)
    def _(i):
        @pl.when(i + 1 < chunks)
        def _():
            last_hop(i + 1)

        coarse_lags(2 * i + 1, cbuf[1])
        coarse_products(2 * i, cbuf[0])
        coarse_lags(jnp.minimum(2 * i + 2, csteps - 1), cbuf[0])
        coarse_products(2 * i + 1, cbuf[1])

    coarse_copies = freq_copies(((cacc, crecv),), cx_send, cx_recv)
    for copy in coarse_copies:
        copy.start()

    row_at = lax.broadcasted_iota(I32, (rows, 128), 0)
    shift = jnp.zeros((rows, 128), I32)
    for b in range(nb):
        block = [trig[p % top_count, b * seg_dev + p // top_count] for p in range(pairs)]
        taken = jnp.int32(0)
        for p in range(pairs):
            hit = block[p] == me
            offset = offs[p % top_count, b * seg_dev + p // top_count]
            shift = jnp.where(
                row_at == jnp.where(hit, b * CAP + taken, -1), offset, shift
            )
            taken = taken + hit.astype(I32)
    lane = lax.broadcasted_iota(I32, (rows, 128), 1)
    tiles = fbins // 128
    lane_angle = ((shift * lane) & (period - 1)).astype(F32) * (2.0 * math.pi / period)
    lane_cos, lane_sin = jnp.cos(lane_angle), jnp.sin(lane_angle)
    coarse_period = period // 128
    tile_at = lax.broadcasted_iota(I32, (rows, tiles), 1) + fme * tiles
    wide = jnp.concatenate([shift] * (tiles // 128), axis=1)
    tile_angle = ((wide * tile_at) & (coarse_period - 1)).astype(F32) * (
        2.0 * math.pi / coarse_period
    )
    tile_cos, tile_sin = jnp.cos(tile_angle), jnp.sin(tile_angle)

    def fine_lags(i, buf):
        per = kf // 128
        turn = lax.rem(tiles - i * per, tiles)
        here_cos = pltpu.roll(tile_cos, turn, 1)
        here_sin = pltpu.roll(tile_sin, turn, 1)
        sub = 512
        for c in range(0, kf, sub):
            window = pl.ds(pl.multiple_of(i * kf + c, sub), sub)
            blocks = [slots[b, :, window].astype(F32) for b in range(nb)]
            w = fw[:, window]
            real = jnp.concatenate([x[:CAP] for x in blocks], axis=0) * w
            imag = jnp.concatenate([x[CAP:] for x in blocks], axis=0) * w
            turn_re, turn_im = [], []
            for t in range(c // 128, (c + sub) // 128):
                a_cos = here_cos[:, t : t + 1]
                a_sin = here_sin[:, t : t + 1]
                turn_re.append(a_cos * lane_cos - a_sin * lane_sin)
                turn_im.append(a_cos * lane_sin + a_sin * lane_cos)
            sr = jnp.concatenate(turn_re, axis=1)
            si = jnp.concatenate(turn_im, axis=1)
            real, imag = real * sr - imag * si, real * si + imag * sr
            held = []

            def emit(j, re, im):
                held.append((re, im))
                if len(held) == 2:
                    low, high = (j - 1) * rows, (j + 1) * rows
                    buf[low:high, c : c + sub] = jnp.concatenate(
                        [held[0][0], held[1][0]], axis=0
                    ).astype(BF16)
                    buf[nfl + low : nfl + high, c : c + sub] = jnp.concatenate(
                        [held[0][1], held[1][1]], axis=0
                    ).astype(BF16)
                    held.clear()

            lag_series(real, imag, fstep[0:1, window], fstep[1:2, window], LF, emit)

    def fine_products(i, buf):
        window = win(i, kf)
        left = jnp.concatenate([ftemp_v[0, 0, :, window], ftemp_v[1, 0, :, window]], axis=0)
        facc[...] += nt_dot(left, buf[...])

    def slots_here(copy, at):
        for d in range(1, nb):
            copy(d, at).wait_recv()

    slots_here(slot_couple, 0)
    fine_lags(0, fl0)

    @pl.loop(0, fsteps // 2 - 1)
    def _(i):
        @pl.when(i + 1 < couples)
        def _():
            slots_here(slot_couple, i + 1)

        @pl.when(i + 1 == couples)
        def _():
            slots_here(slot_last, 0)

        fine_lags(2 * i + 1, fl1)
        fine_products(2 * i, fl0)
        fine_lags(2 * i + 2, fl0)
        fine_products(2 * i + 1, fl1)

    slots_here(slot_last, 1)
    fine_lags(fsteps - 1, fl1)
    fine_products(fsteps - 2, fl0)
    fine_products(fsteps - 1, fl1)

    both = facc.shape[0] // 2
    re = facc[:both, :nfl] + facc[both:, nfl:]
    im = facc[:both, nfl:] - facc[both:, :nfl]
    for k in range(nf):
        fsum[k, 0] = re[k * q : (k + 1) * q]
        fsum[k, 1] = im[k * q : (k + 1) * q]
    fine_copies = freq_copies(((fsum, frecv),), fx_send, fx_recv)
    for copy in fine_copies:
        copy.start()
    for copy in norm_copies + fine_copies:
        copy.wait_recv()
    def whole_norm(parts):
        shares = []
        for s in range(parts.shape[1]):
            total = parts[0, s]
            for x in range(1, nf):
                total = total + parts[x, s]
            shares.append(total)
        return jnp.sum(jnp.concatenate(shares, axis=0), axis=1, keepdims=True)

    re, im = fsum[fme, 0], fsum[fme, 1]
    for d in range(nf - 1):
        re = re + frecv[d, 0]
        im = im + frecv[d, 1]
    ratio = jnp.transpose((re * re + im * im) / whole_norm(fnall))
    fsnr[...] = jnp.max(ratio.reshape(LF, rows, q), axis=0)
    bcopies = back_copies()
    for copy in bcopies:
        copy.start()
    back[me] = fsnr[...]

    for copy in coarse_copies:
        copy.wait_recv()
    acc = cacc[fme]
    for d in range(nf - 1):
        acc = acc + crecv[d]
    re, im = acc[:, :nc], acc[:, nc:]
    top = peak(re * re + im * im, segs)
    csnr[...] = jnp.transpose(top[:, :128] / whole_norm(cnall))[:segs]

    for copy in coarse_copies + norm_copies + fine_copies:
        copy.wait_send()
    for hop in range(nb - 1):
        for c in range(chunks):

            @pl.when(has_right & (me - hop >= 0))
            def _():
                ag_right(hop, c).wait_send()

            @pl.when(has_left & (me + hop < nb))
            def _():
                ag_left(hop, c).wait_send()

    @pl.loop(0, couples)
    def _(g):
        for d in range(1, nb):
            slot_couple(d, g).wait_send()

    for k in range(2):
        for d in range(1, nb):
            slot_last(d, k).wait_send()

    for copy in bcopies:
        copy.wait()
    for p in range(pairs):
        bank = jnp.clip(own[p], 0, nb - 1)
        row = me * CAP + jnp.minimum(own_rank[p], CAP - 1)
        fout[p : p + 1, :] = back[bank, pl.ds(row, 1), :]


def body(
    coarse_spectra,
    fine_spectra,
    coarse_templates,
    fine_templates,
    coarse_weight,
    fine_weight,
    triggers,
    offsets,
):
    nb = lax.axis_size("bank")
    nf = lax.axis_size("freq")
    ns = lax.axis_size("seg")
    seg_local = fine_spectra.shape[0]
    cbins = coarse_spectra.shape[2]
    fbins = fine_spectra.shape[2]
    top_count = triggers.shape[1]
    sub_width = fine_templates.shape[2]
    ctemps = coarse_templates.shape[1]
    rows = nb * CAP
    segs = nb * seg_local
    kc = min(1024, cbins // 2)
    kf = min(2048, fbins // 2)
    chunks = cbins // kc // 2
    csteps = cbins // kc
    fsteps = fbins // kf
    crow = ctemps // nf
    q = sub_width // nf
    period = 2 * fbins * nf
    fsplit = ns if q // ns % 16 == 0 else 1
    assert period & (period - 1) == 0 and csteps % 2 == 0 and fsteps % 2 == 0
    nc = segs * LC
    nfl = rows * LF
    ctable = jnp.asarray(unit_table(cbins * nf, CSTRIDE, 2 * cbins * nf))
    ftable = jnp.asarray(unit_table(fbins * nf, 1, period))

    vmem, anywhere = pl.BlockSpec(memory_space=pltpu.VMEM), pl.BlockSpec(memory_space=pl.ANY)
    dma = pltpu.SemaphoreType.DMA
    lag_buf = pltpu.VMEM((nc, kc), BF16)
    fine_buf = pltpu.VMEM((2 * nfl, kf), BF16)
    csnr, fine_rows = pl.pallas_call(
        functools.partial(kernel, (nb, nf, ns, fsplit, kc, kf, chunks, period)),
        out_shape=(
            pltpu.VMEM((segs, crow), F32),
            pltpu.VMEM((seg_local * top_count, q), F32),
        ),
        in_specs=[anywhere] * 10,
        out_specs=(vmem, vmem),
        scratch_shapes=[
            pltpu.SMEM((top_count, triggers.shape[0]), I32),
            pltpu.SMEM((top_count, triggers.shape[0]), I32),
            pltpu.VMEM(coarse_spectra.shape, BF16),
            pltpu.VMEM(fine_spectra.shape, BF16),
            pltpu.VMEM(coarse_templates.shape, BF16),
            pltpu.VMEM(fine_templates.shape, BF16),
            pltpu.VMEM((1, cbins), F32),
            pltpu.VMEM((1, fbins), F32),
            pltpu.VMEM((2, cbins), F32),
            pltpu.VMEM((2, fbins), F32),
            pltpu.VMEM((nb, 2 * seg_local, cbins), BF16),
            pltpu.VMEM((nb, 2 * CAP, fbins), BF16),
            pltpu.VMEM((nb, 2 * CAP, fbins), BF16),
            lag_buf, lag_buf, lag_buf, lag_buf, lag_buf, lag_buf,
            fine_buf, fine_buf,
            pltpu.VMEM((nf, crow, 2 * nc), F32),
            pltpu.VMEM((nf, crow // ns, 128), F32),
            pltpu.VMEM((nf, ns, crow // ns, 128), F32),
            pltpu.VMEM((2 * sub_width, 2 * nfl), F32),
            pltpu.VMEM((nf, 2, q, nfl), F32),
            pltpu.VMEM((nf, q // fsplit, 128), F32),
            pltpu.VMEM((nf, fsplit, q // fsplit, 128), F32),
            pltpu.VMEM((rows, q), F32),
            pltpu.VMEM((nb, rows, q), F32),
            pltpu.VMEM((nf - 1, crow, 2 * nc), F32),
            pltpu.VMEM((nf - 1, 2, q, nfl), F32),
            dma((8,)),
            dma((csteps,)),
            dma((fsteps,)),
            dma((nb - 1, chunks)),
            dma((nb - 1, chunks)),
            dma((nb - 1, chunks)),
            dma((nb - 1, chunks)),
            dma((nb - 1, fsteps // 2 + 1)),
            dma((nb - 1, fsteps // 2 + 1)),
            dma((nf - 1, 1)),
            dma((nf - 1, 1)),
            dma((nf * ns, 2)),
            dma((nf * ns, 2)),
            dma((nf - 1, 1)),
            dma((nf - 1, 1)),
            dma((nb - 1,)),
            dma((nb - 1,)),
        ],
        compiler_params=pltpu.CompilerParams(
            collective_id=0,
            has_side_effects=True,
            vmem_limit_bytes=60 * 1024 * 1024,
        ),
    )(
        triggers.T,
        offsets.T,
        coarse_spectra,
        fine_spectra,
        coarse_templates,
        fine_templates,
        coarse_weight[None, :],
        fine_weight[None, :],
        ctable,
        ftable,
    )
    def settle(c_in, f_in, c_out, f_out, sem):
        copies = [
            pltpu.make_async_copy(c_in, c_out, sem.at[0]),
            pltpu.make_async_copy(f_in, f_out, sem.at[1]),
        ]
        for copy in copies:
            copy.start()
        for copy in copies:
            copy.wait()

    csnr, fine_rows = pl.pallas_call(
        settle,
        out_shape=(
            jax.ShapeDtypeStruct(csnr.shape, F32), jax.ShapeDtypeStruct(fine_rows.shape, F32)
        ),
        in_specs=[vmem, vmem],
        out_specs=(anywhere, anywhere),
        scratch_shapes=[dma((2,))],
    )(
        pltpu.with_memory_space_constraint(csnr, pltpu.VMEM),
        pltpu.with_memory_space_constraint(fine_rows, pltpu.VMEM),
    )
    return (csnr.T, fine_rows.reshape(seg_local, top_count, q))


def solution(mesh):
    return jax.shard_map(
        body,
        mesh=mesh,
        in_specs=(
            P(("groups", "seg", "bank"), None, "freq"),
            P(("groups", "seg", "bank"), None, "freq"),
            P(None, "bank", "freq"),
            P(None, "bank", None, "freq"),
            P(("groups", "freq")),
            P(("groups", "freq")),
            P(("groups", "seg"), None),
            P(("groups", "seg"), None),
        ),
        out_specs=(
            P(("bank", "freq"), ("groups", "seg")),
            P(("groups", "seg", "bank"), None, "freq"),
        ),
        check_vma=False,
    )
```
